256 devices in a mesh: row: 128 (over z, y, x), width: 2 (over core).
Axes of the slice: x: 4, y: 4, z: 8, core: 2. Of those that a mesh axis runs over, the one named last changes fastest.
Arguments:
- row_numbers: int32 [4096, 2], P('row'), may hold values from 0 to 131071
- item_table: bfloat16 [131072, 64], P('row', 'width'), may hold values from -6 to 6
- dense_part: float32 [4096, 64], P('row', 'width'), may hold values from -6 to 6
- small_ids: int32 [4096], P('row'), may hold values from 0 to 255
- small_table: bfloat16 [256, 64], P('row', 'width'), may hold values from -6 to 6
Outputs:
- features: bfloat16 [4096, 3, 64], P('row', None, 'width')
The draws below stay inside these ranges and needn't reach their ends.
All inputs are finite; a program needn't handle non-finite values.
Results may differ from the reference program's by a relative error of at most 0.0004.
Values may be sent and summed in bfloat16 or wider, within the bound.
A program may use at most 64 MiB of HBM per device.

```python
import math
import jax
import jax.numpy as jnp
import numpy as np

EXAMPLES = 4096
FEATURES = 64
PICKS = 2
BIG_ROWS = 131072
SMALL_ROWS = 256


def place_ends(entries, stream_key, least, largest):
    spot = [jax.random.randint(jax.random.fold_in(stream_key, axis), (), 0, length) for axis, length in enumerate(entries.shape)]
    widest = entries.shape.index(max(entries.shape))
    neighbour = spot[:widest] + [(spot[widest] + 1) % entries.shape[widest]] + spot[widest + 1:]
    return entries.at[tuple(spot)].set(least).at[tuple(neighbour)].set(largest)


def block_levels(rng, dims, split, low, top_value):
    loudness, own = 1.0, jax.random.fold_in(rng, 6)
    for dim, blocks in split:
        heights = jnp.exp(jax.random.uniform(jax.random.fold_in(own, dim), (blocks,), jnp.float32, low / len(split), top_value / len(split)))
        loudness = loudness * jnp.repeat(heights, dims[dim] // blocks).reshape([-1 if axis == dim else 1 for axis in range(len(dims))])
    return loudness


def wide_ids(key, shape, amount, skew):
    portions = [min(1 << octave, amount + 1 - (1 << octave)) * (1 << 20) // math.isqrt((1 << octave) ** skew) + 1 for octave in range((amount + 1).bit_length()) if 1 << octave <= amount]
    spread = 1 + sum(portions) // (1 << 30)
    table = np.cumsum(np.array([max(1, weight // spread) for weight in portions]))
    lot = jax.random.randint(jax.random.fold_in(key, 1), shape, 0, int(table[len(portions) - 1]))
    start = jnp.left_shift(1, jnp.searchsorted(jnp.asarray(table, jnp.int32), lot, side="right").astype(jnp.int32))
    standing = start - 1 + jax.random.randint(jax.random.fold_in(key, 4), shape, 0, 1 << 30) % jnp.minimum(start, amount + 1 - start)
    return jax.random.permutation(jax.random.fold_in(key, 2), amount)[standing].astype(jnp.int32)


def noise(stream_key, extent, deviation, most, shards=(), kind=jnp.bfloat16):
    values = deviation * jax.random.normal(stream_key, extent, jnp.float32)
    if shards:
        values = values * block_levels(stream_key, extent, shards, -0.22, 0.18)
    return jnp.clip(values, -most, most).astype(kind)


def setup_inputs(seed: int = 0) -> dict:
    splits = jax.random.split(jax.random.key(seed), 6)
    row_numbers = place_ends(wide_ids(splits[0], (EXAMPLES, PICKS), BIG_ROWS, 2), jax.random.fold_in(splits[0], 3), 0, BIG_ROWS - 1).astype(jnp.int32)
    item_table = noise(splits[1], (BIG_ROWS, FEATURES), 1.0, 6.0, ((0, 128), (1, 2)))
    dense_part = noise(splits[2], (EXAMPLES, FEATURES), 1.0, 6.0, ((0, 128), (1, 2)), jnp.float32)
    small_ids = place_ends(jax.random.randint(splits[3], (EXAMPLES,), 0, SMALL_ROWS), jax.random.fold_in(splits[3], 1), 0, SMALL_ROWS - 1).astype(jnp.int32)
    small_table = noise(splits[4], (SMALL_ROWS, FEATURES), 1.0, 6.0, ((0, 128), (1, 2)))
    return {"row_numbers": row_numbers, "item_table": item_table, "dense_part": dense_part, "small_ids": small_ids, "small_table": small_table}


def reference(row_numbers, item_table, dense_part, small_ids, small_table):
    pooled = jnp.sum(item_table[row_numbers].astype(jnp.float32), axis=1) * PICKS ** -0.5
    small_rows = small_table[small_ids].astype(jnp.float32)
    features = jnp.stack([dense_part, pooled, small_rows], axis=1).astype(jnp.bfloat16)
    return features
```

```python
import functools

import jax
import jax.numpy as jnp
from jax import lax
from jax.experimental import pallas as pl
from jax.experimental.pallas import tpu as pltpu
from jax.sharding import Mesh
from jax.sharding import PartitionSpec as P

ROW = ("row_0", "row_1", "row_2")
NZ, NY, NX = 8, 4, 4
MESH = pl.DeviceIdType.MESH
OFFSETS = sorted(
    ((kz, ky) for kz in range(NZ) for ky in range(NY)),
    key=lambda k: (min(k[0], NZ - k[0]) + min(k[1], NY - k[1]), k),
)
SLOT = {k: i for i, k in enumerate(OFFSETS)}
BACK = [SLOT[(-kz % NZ, -ky % NY)] for kz, ky in OFFSETS]
PEERS = len(OFFSETS)
ROWS = 1024
LOW = 256
HIGH = ROWS // LOW
EX = 32
F = 32


def kernel(
    ids_hbm, table_hbm, dense_hbm, sid_hbm, small_hbm, out_ref,
    ids_in, dense, sid, small_in, msg, ids, tab, send, recv, small,
    local_sem, tab_send, tab_recv, ids_send, ids_recv, row_send, row_recv,
    sx_send, sx_recv, sp_send, sp_recv,
):
    z, y, x, w = (lax.axis_index(name) for name in (*ROW, "width"))

    def plane_peer(slot):
        kz, ky = OFFSETS[slot]
        return (lax.rem(z + kz, NZ), lax.rem(y + ky, NY), x, w)

    def x_peer(k):
        return (z, y, lax.rem(x + k, NX), w)

    barrier = pltpu.get_barrier_semaphore()
    for k in range(1, NX):
        pl.semaphore_signal(barrier, inc=1, device_id=x_peer(k), device_id_type=MESH)
    for slot in range(PEERS - 1, 0, -1):
        pl.semaphore_signal(barrier, inc=1, device_id=plane_peer(slot), device_id_type=MESH)

    fetches = [
        pltpu.make_async_copy(src, dst, local_sem.at[i])
        for i, (src, dst) in enumerate(
            (
                (ids_hbm, ids_in), (small_hbm, small_in), (table_hbm, tab.at[0]),
                (sid_hbm, sid), (dense_hbm, dense),
            )
        )
    ]
    for fetch in fetches:
        fetch.start()

    group = z * NY + y
    fetches[0].wait()
    pair = ids_in[...]
    line = jnp.concatenate([pair[0:1], pair[1:2], pair[0:1], pair[1:2]], axis=1)
    msg[...] = line
    ids[0:1, :] = line
    fetches[1].wait()
    my_small = small.at[pl.ds(group * 8 + x * 2, 2)]
    my_small[...] = small_in[...].astype(jnp.float32)
    fetches[2].wait()

    pl.semaphore_wait(barrier, PEERS - 1 + NX - 1)

    def remote(src, dst, s, r, peer):
        return pltpu.make_async_remote_copy(
            src_ref=src, dst_ref=dst, send_sem=s, recv_sem=r, device_id=peer, device_id_type=MESH
        )

    id_copies = {
        slot: remote(
            msg, ids.at[pl.ds(BACK[slot], 1)], ids_send.at[slot], ids_recv.at[BACK[slot]],
            plane_peer(slot),
        )
        for slot in range(1, PEERS)
    }
    sx_copies = [
        remote(my_small, my_small, sx_send.at[k], sx_recv.at[NX - k], x_peer(k))
        for k in range(1, NX)
    ]
    tab_copies = [
        remote(tab.at[0], tab.at[NX - k], tab_send.at[k], tab_recv.at[NX - k], x_peer(k))
        for k in range(1, NX)
    ]
    for slot in range(PEERS - 1, 0, -1):
        id_copies[slot].start()
    for copy in sx_copies:
        copy.start()
    for copy in tab_copies:
        copy.start()

    for copy in sx_copies:
        copy.wait_recv()
    my_eight = small.at[pl.ds(pl.multiple_of(group * 8, 8), 8)]
    sp_copies = [
        remote(my_eight, my_eight, sp_send.at[slot], sp_recv.at[BACK[slot]], plane_peer(slot))
        for slot in range(1, PEERS)
    ]
    for copy in reversed(sp_copies):
        copy.start()

    fetches[3].wait()
    fetches[4].wait()
    out_ref[0] = dense[...].astype(jnp.bfloat16)

    for copy in tab_copies:
        copy.wait_recv()
    lhs = jnp.concatenate(
        [tab[j, :, b * LOW : (b + 1) * LOW] for j in range(NX) for b in range(HIGH)], axis=0
    )
    lane = lax.broadcasted_iota(jnp.int32, (1, 128), 1)
    low_half = lane < 64
    low_half16 = lax.broadcasted_iota(jnp.int32, (16, 128), 1) < 64
    base = group * (NX * ROWS)
    low_rows = lax.broadcasted_iota(jnp.int32, (LOW, 4 * 64), 0)

    row_copies = []
    for first in range(0, PEERS, 4):
        slots = range(first, first + 4)
        for slot in slots:
            if slot:
                id_copies[BACK[slot]].wait_recv()
        lines = [ids[slot : slot + 1, :] for slot in slots]
        wanted = jnp.concatenate(
            [jnp.where(low_half, lines[0], lines[1]), jnp.where(low_half, lines[2], lines[3])],
            axis=1,
        ) - base
        low = wanted & (LOW - 1)
        high = wanted >> 8
        one_hot = jnp.where(low_rows == low, 1.0, 0.0).astype(jnp.bfloat16)
        found = jnp.dot(lhs, one_hot, preferred_element_type=jnp.float32)
        rows = jnp.zeros((F, 4 * 64), jnp.float32)
        for j in range(NX):
            owner = lax.rem(x + j, NX)
            for b in range(HIGH):
                at = (j * HIGH + b) * F
                rows = jnp.where(high == owner * HIGH + b, found[at : at + F], rows)
        for half in range(2):
            part = rows[:, half * 128 : (half + 1) * 128]
            upper, lower = part[:16], part[16:]
            turned_upper = pltpu.roll(upper, 64, 1)
            turned_lower = pltpu.roll(lower, 64, 1)
            even = jnp.where(low_half16, upper, turned_lower).astype(jnp.bfloat16)
            odd = jnp.where(low_half16, turned_upper, lower).astype(jnp.bfloat16)
            for slot, block in ((first + 2 * half, even), (first + 2 * half + 1, odd)):
                if slot == 0:
                    recv[0] = block
                    continue
                send[slot] = block
                copy = remote(
                    send.at[slot], recv.at[BACK[slot]], row_send.at[slot],
                    row_recv.at[BACK[slot]], plane_peer(slot),
                )
                copy.start()
                row_copies.append(copy)

    for copy in sp_copies:
        copy.wait_recv()
    small_hot = jnp.where(
        lax.broadcasted_iota(jnp.int32, (256, EX), 0) == sid[...], 1.0, 0.0
    ).astype(jnp.bfloat16)
    out_ref[2] = lax.dot_general(
        small_hot, small[...].astype(jnp.bfloat16), (((0,), (0,)), ((), ())),
        preferred_element_type=jnp.float32,
    ).astype(jnp.bfloat16)

    for copy in tab_copies + sx_copies + sp_copies + list(id_copies.values()):
        copy.wait_send()
    for copy in row_copies:
        copy.wait_send()
    for copy in row_copies:
        copy.wait_recv()

    total = recv[0].astype(jnp.float32)
    for slot in range(1, PEERS):
        total = total + recv[slot].astype(jnp.float32)
    both = jnp.concatenate(
        [jnp.where(low_half16, total, 0.0), jnp.where(low_half16, 0.0, total)], axis=0
    ).astype(jnp.bfloat16)
    example = lax.broadcasted_iota(jnp.int32, (EX, 128), 0)
    spot = lax.broadcasted_iota(jnp.int32, (EX, 128), 1)
    picks = jnp.where((spot & (EX - 1)) == example, 1.0, 0.0).astype(jnp.bfloat16)
    pooled = lax.dot_general(
        picks, both, (((1,), (1,)), ((), ())), preferred_element_type=jnp.float32
    )
    out_ref[1] = (pooled * 2 ** (-0.5)).astype(jnp.bfloat16)


def shards(row_numbers, item_table, dense_part, small_ids, small_table):
    any_space = pl.BlockSpec(memory_space=pl.ANY)
    dma = pltpu.SemaphoreType.DMA
    parts = pl.pallas_call(
        kernel,
        out_shape=jax.ShapeDtypeStruct((3, EX, F), jnp.bfloat16),
        in_specs=[any_space] * 5,
        out_specs=pl.BlockSpec(memory_space=pltpu.VMEM),
        scratch_shapes=[
            pltpu.VMEM((2, EX), jnp.int32),
            pltpu.VMEM((EX, F), jnp.float32),
            pltpu.VMEM((1, EX), jnp.int32),
            pltpu.VMEM((2, F), jnp.bfloat16),
            pltpu.VMEM((1, 128), jnp.int32),
            pltpu.VMEM((PEERS, 128), jnp.int32),
            pltpu.VMEM((NX, F, ROWS), jnp.bfloat16),
            pltpu.VMEM((PEERS, 16, 128), jnp.bfloat16),
            pltpu.VMEM((PEERS, 16, 128), jnp.bfloat16),
            pltpu.VMEM((256, F), jnp.float32),
            dma((5,)), dma((NX,)), dma((NX,)), dma((PEERS,)), dma((PEERS,)),
            dma((PEERS,)), dma((PEERS,)), dma((NX,)), dma((NX,)), dma((PEERS,)), dma((PEERS,)),
        ],
        compiler_params=pltpu.CompilerParams(collective_id=0, has_side_effects=True),
    )(row_numbers.T, item_table.T, dense_part, small_ids.reshape(1, EX), small_table)
    return parts.transpose(1, 0, 2)


def solution(mesh):
    torus = Mesh(mesh.devices.reshape(NZ, NY, NX, 2), (*ROW, "width"))
    return jax.shard_map(
        shards,
        mesh=torus,
        in_specs=(P(ROW, None), P(ROW, "width"), P(ROW, "width"), P(ROW), P(ROW, "width")),
        out_specs=P(ROW, None, "width"),
        check_vma=False,
    )
```

```python
import functools

import jax
import jax.numpy as jnp
from jax import lax
from jax.experimental import pallas as pl
from jax.experimental.pallas import tpu as pltpu
from jax.sharding import Mesh
from jax.sharding import PartitionSpec as P

ROW = ("row_0", "row_1", "row_2")
NZ, NY, NX = 8, 4, 4
MESH = pl.DeviceIdType.MESH
OFFSETS = sorted(
    ((kz, ky) for kz in range(NZ) for ky in range(NY)),
    key=lambda k: (min(k[0], NZ - k[0]) + min(k[1], NY - k[1]), k),
)
SLOT = {k: i for i, k in enumerate(OFFSETS)}
BACK = [SLOT[(-kz % NZ, -ky % NY)] for kz, ky in OFFSETS]
PEERS = len(OFFSETS)
ROWS = 1024
LOW = 256
HIGH = ROWS // LOW
EX = 32
F = 32


CHUNKS = 4
PER = PEERS // CHUNKS
WIDE = PER * 64


def kernel(
    ids_hbm, table_hbm, dense_hbm, sid_hbm, small_hbm, out_ref,
    ids_in, dense, sid, small_in, msg, ids, tab, hot, highs, sums, send, recv, small,
    local_sem, tab_send, tab_recv, ids_send, ids_recv, row_send, row_recv,
    sx_send, sx_recv, sp_send, sp_recv,
):
    z, y, x, w = (lax.axis_index(name) for name in (*ROW, "width"))

    def plane_peer(slot):
        kz, ky = OFFSETS[slot]
        return (lax.rem(z + kz, NZ), lax.rem(y + ky, NY), x, w)

    def x_peer(k):
        return (z, y, lax.rem(x + k, NX), w)

    barrier = pltpu.get_barrier_semaphore()
    for slot in range(PEERS - 1, 0, -1):
        pl.semaphore_signal(barrier, inc=1, device_id=plane_peer(slot), device_id_type=MESH)
    for k in range(1, NX):
        pl.semaphore_signal(barrier, inc=1, device_id=x_peer(k), device_id_type=MESH)

    fetches = [
        pltpu.make_async_copy(src, dst, local_sem.at[i])
        for i, (src, dst) in enumerate(
            (
                (ids_hbm, ids_in), (small_hbm, small_in), (table_hbm, tab.at[0]),
                (sid_hbm, sid), (dense_hbm, dense),
            )
        )
    ]
    for fetch in fetches:
        fetch.start()

    group = z * NY + y
    fetches[0].wait()
    pair = ids_in[...]
    line = jnp.concatenate([pair[0:1], pair[1:2], pair[0:1], pair[1:2]], axis=1)
    msg[...] = line
    ids[0:1, :] = line
    fetches[1].wait()
    my_small = small.at[x, pl.ds(group * 2, 2)]
    my_small[...] = small_in[...].astype(jnp.float32)
    fetches[2].wait()
    fetches[3].wait()
    fetches[4].wait()
    out_ref[0] = dense[...].astype(jnp.bfloat16)

    pl.semaphore_wait(barrier, PEERS - 1 + NX - 1)

    def remote(src, dst, s, r, peer):
        return pltpu.make_async_remote_copy(
            src_ref=src, dst_ref=dst, send_sem=s, recv_sem=r, device_id=peer, device_id_type=MESH
        )

    id_copies = {
        slot: remote(
            msg, ids.at[pl.ds(BACK[slot], 1)], ids_send.at[slot], ids_recv.at[BACK[slot]],
            plane_peer(slot),
        )
        for slot in range(1, PEERS)
    }
    sp_copies = {
        slot: remote(
            my_small, my_small, sp_send.at[slot], sp_recv.at[BACK[slot]], plane_peer(slot)
        )
        for slot in range(1, PEERS)
    }
    tab_copies = [
        remote(tab.at[0], tab.at[NX - k], tab_send.at[k], tab_recv.at[NX - k], x_peer(k))
        for k in range(1, NX)
    ]
    for copy in tab_copies:
        copy.start()
    for slot in range(PEERS - 1, 0, -1):
        id_copies[slot].start()
    for slot in range(PEERS - 1, 0, -1):
        sp_copies[slot].start()

    lane = lax.broadcasted_iota(jnp.int32, (1, 128), 1)
    low_half = lane < 64
    low_half16 = lax.broadcasted_iota(jnp.int32, (16, 128), 1) < 64
    base = group * (NX * ROWS)
    low_rows = lax.broadcasted_iota(jnp.int32, (LOW, WIDE), 0)

    def look_up(chunk, j, rows):
        lhs = jnp.concatenate(
            [tab[j, :, b * LOW : (b + 1) * LOW] for b in range(HIGH)], axis=0
        )
        found = jnp.dot(lhs, hot[chunk], preferred_element_type=jnp.float32)
        high = highs[chunk]
        owner = lax.rem(x + j, NX)
        for b in range(HIGH):
            rows = jnp.where(high == owner * HIGH + b, found[b * F : (b + 1) * F], rows)
        return rows

    for chunk in range(CHUNKS):
        slots = range(chunk * PER, (chunk + 1) * PER)
        for slot in slots:
            if slot:
                id_copies[BACK[slot]].wait_recv()
        lines = [ids[slot : slot + 1, :] for slot in slots]
        wanted = jnp.concatenate(
            [jnp.where(low_half, a, b) for a, b in zip(lines[::2], lines[1::2])], axis=1
        ) - base
        highs[chunk] = wanted >> 8
        hot[chunk] = jnp.where(low_rows == (wanted & (LOW - 1)), 1.0, 0.0).astype(jnp.bfloat16)
        sums[chunk] = look_up(chunk, 0, jnp.zeros((F, WIDE), jnp.float32))

    for slot in range(1, PEERS):
        sp_copies[slot].wait_recv()
    sx_copies = [
        remote(small.at[x], small.at[x], sx_send.at[k], sx_recv.at[NX - k], x_peer(k))
        for k in range(1, NX)
    ]
    for copy in sx_copies:
        copy.start()

    for j in (1, 3):
        tab_copies[NX - j - 1].wait_recv()
        for chunk in range(CHUNKS):
            sums[chunk] = look_up(chunk, j, sums[chunk])
    tab_copies[1].wait_recv()
    row_copies = []
    for chunk in range(CHUNKS - 1, -1, -1):
        rows = look_up(chunk, 2, sums[chunk])
        for half in range(PER // 2):
            part = rows[:, half * 128 : (half + 1) * 128]
            upper, lower = part[:16], part[16:]
            turned_upper = pltpu.roll(upper, 64, 1)
            turned_lower = pltpu.roll(lower, 64, 1)
            even = jnp.where(low_half16, upper, turned_lower).astype(jnp.bfloat16)
            odd = jnp.where(low_half16, turned_upper, lower).astype(jnp.bfloat16)
            slot = chunk * PER + 2 * half
            if slot:
                send[slot] = even
            else:
                recv[0] = even
            send[slot + 1] = odd
        for slot in range((chunk + 1) * PER - 1, max(chunk * PER, 1) - 1, -1):
            copy = remote(
                send.at[slot], recv.at[BACK[slot]], row_send.at[slot],
                row_recv.at[BACK[slot]], plane_peer(slot),
            )
            copy.start()
            row_copies.append(copy)

    for copy in sx_copies:
        copy.wait_recv()
    wanted = sid[...]
    place = ((wanted >> 1) & (NX - 1)) * 64 + (wanted >> 3) * 2 + (wanted & 1)
    small_hot = jnp.where(
        lax.broadcasted_iota(jnp.int32, (256, EX), 0) == place, 1.0, 0.0
    ).astype(jnp.bfloat16)
    small_rows = jnp.concatenate([small[k] for k in range(NX)], axis=0).astype(jnp.bfloat16)
    out_ref[2] = lax.dot_general(
        small_hot, small_rows, (((0,), (0,)), ((), ())), preferred_element_type=jnp.float32
    ).astype(jnp.bfloat16)

    for copy in tab_copies + sx_copies + list(sp_copies.values()) + list(id_copies.values()):
        copy.wait_send()
    for copy in row_copies:
        copy.wait_send()
    for copy in row_copies:
        copy.wait_recv()

    total = recv[0].astype(jnp.float32)
    for slot in range(1, PEERS):
        total = total + recv[slot].astype(jnp.float32)
    both = jnp.concatenate(
        [jnp.where(low_half16, total, 0.0), jnp.where(low_half16, 0.0, total)], axis=0
    ).astype(jnp.bfloat16)
    example = lax.broadcasted_iota(jnp.int32, (EX, 128), 0)
    spot = lax.broadcasted_iota(jnp.int32, (EX, 128), 1)
    picks = jnp.where((spot & (EX - 1)) == example, 1.0, 0.0).astype(jnp.bfloat16)
    pooled = lax.dot_general(
        picks, both, (((1,), (1,)), ((), ())), preferred_element_type=jnp.float32
    )
    out_ref[1] = (pooled * 2 ** (-0.5)).astype(jnp.bfloat16)


def shards(row_numbers, item_table, dense_part, small_ids, small_table):
    dma = pltpu.SemaphoreType.DMA
    parts = pl.pallas_call(
        kernel,
        out_shape=jax.ShapeDtypeStruct((3, EX, F), jnp.bfloat16),
        in_specs=[pl.BlockSpec(memory_space=pltpu.HBM)] * 5,
        out_specs=pl.BlockSpec(memory_space=pltpu.VMEM),
        scratch_shapes=[
            pltpu.VMEM((2, EX), jnp.int32),
            pltpu.VMEM((EX, F), jnp.float32),
            pltpu.VMEM((1, EX), jnp.int32),
            pltpu.VMEM((2, F), jnp.bfloat16),
            pltpu.VMEM((1, 128), jnp.int32),
            pltpu.VMEM((PEERS, 128), jnp.int32),
            pltpu.VMEM((NX, F, ROWS), jnp.bfloat16),
            pltpu.VMEM((CHUNKS, LOW, WIDE), jnp.bfloat16),
            pltpu.VMEM((CHUNKS, 1, WIDE), jnp.int32),
            pltpu.VMEM((CHUNKS, F, WIDE), jnp.float32),
            pltpu.VMEM((PEERS, 16, 128), jnp.bfloat16),
            pltpu.VMEM((PEERS, 16, 128), jnp.bfloat16),
            pltpu.VMEM((NX, 2 * PEERS, F), jnp.float32),
            dma((5,)), dma((NX,)), dma((NX,)), dma((PEERS,)), dma((PEERS,)),
            dma((PEERS,)), dma((PEERS,)), dma((NX,)), dma((NX,)), dma((PEERS,)), dma((PEERS,)),
        ],
        compiler_params=pltpu.CompilerParams(
            collective_id=0, has_side_effects=True, vmem_limit_bytes=16 * 2**20
        ),
    )(row_numbers.T, item_table.T, dense_part, small_ids.reshape(1, EX), small_table)
    return parts.transpose(1, 0, 2)


def solution(mesh):
    torus = Mesh(mesh.devices.reshape(NZ, NY, NX, 2), (*ROW, "width"))
    return jax.shard_map(
        shards,
        mesh=torus,
        in_specs=(P(ROW, None), P(ROW, "width"), P(ROW, "width"), P(ROW), P(ROW, "width")),
        out_specs=P(ROW, None, "width"),
        check_vma=False,
    )
```

```python
import functools

import jax
import jax.numpy as jnp
from jax import lax
from jax.experimental import pallas as pl
from jax.experimental.pallas import tpu as pltpu
from jax.sharding import Mesh
from jax.sharding import PartitionSpec as P

ROW = ("row_0", "row_1", "row_2")
NZ, NY, NX = 8, 4, 4
MESH = pl.DeviceIdType.MESH
OFFSETS = sorted(
    ((kz, ky) for kz in range(NZ) for ky in range(NY)),
    key=lambda k: (min(k[0], NZ - k[0]) + min(k[1], NY - k[1]), k),
)
SLOT = {k: i for i, k in enumerate(OFFSETS)}
BACK = [SLOT[(-kz % NZ, -ky % NY)] for kz, ky in OFFSETS]
PEERS = len(OFFSETS)
ROWS = 1024
LOW = 256
HIGH = ROWS // LOW
EX = 32
F = 32


CHUNKS = 4
PER = PEERS // CHUNKS
WIDE = PER * 64


def kernel(
    ids_hbm, table_hbm, dense_hbm, sid_hbm, small_hbm, out_ref,
    ids_in, dense, sid, small_in, msg, ids, tab, hot, highs, sums, send, recv, small,
    local_sem, tab_send, tab_recv, ids_send, ids_recv, row_send, row_recv,
    sx_send, sx_recv, sp_send, sp_recv,
):
    z, y, x, w = (lax.axis_index(name) for name in (*ROW, "width"))

    def plane_peer(slot):
        kz, ky = OFFSETS[slot]
        return (lax.rem(z + kz, NZ), lax.rem(y + ky, NY), x, w)

    def x_peer(k):
        return (z, y, lax.rem(x + k, NX), w)

    barrier = pltpu.get_barrier_semaphore()
    for slot in range(PEERS - 1, 0, -1):
        pl.semaphore_signal(barrier, inc=1, device_id=plane_peer(slot), device_id_type=MESH)
    for k in range(1, NX):
        pl.semaphore_signal(barrier, inc=1, device_id=x_peer(k), device_id_type=MESH)

    fetches = [
        pltpu.make_async_copy(src, dst, local_sem.at[i])
        for i, (src, dst) in enumerate(
            (
                (ids_hbm, ids_in), (small_hbm, small_in), (table_hbm, tab.at[0]),
                (sid_hbm, sid), (dense_hbm, dense),
            )
        )
    ]
    for fetch in fetches:
        fetch.start()

    group = z * NY + y
    fetches[0].wait()
    pair = ids_in[...]
    line = jnp.concatenate([pair[0:1], pair[1:2], pair[0:1], pair[1:2]], axis=1)
    msg[...] = line
    ids[0:1, :] = line
    fetches[1].wait()
    my_small = small.at[x, pl.ds(group * 2, 2)]
    my_small[...] = small_in[...].astype(jnp.float32)
    fetches[2].wait()
    fetches[3].wait()
    fetches[4].wait()
    out_ref[0] = dense[...].astype(jnp.bfloat16)

    pl.semaphore_wait(barrier, PEERS - 1 + NX - 1)

    def remote(src, dst, s, r, peer):
        return pltpu.make_async_remote_copy(
            src_ref=src, dst_ref=dst, send_sem=s, recv_sem=r, device_id=peer, device_id_type=MESH
        )

    id_copies = {
        slot: remote(
            msg, ids.at[pl.ds(BACK[slot], 1)], ids_send.at[slot], ids_recv.at[BACK[slot]],
            plane_peer(slot),
        )
        for slot in range(1, PEERS)
    }
    sp_copies = {
        slot: remote(
            my_small, my_small, sp_send.at[slot], sp_recv.at[BACK[slot]], plane_peer(slot)
        )
        for slot in range(1, PEERS)
    }
    tab_copies = [
        remote(tab.at[0], tab.at[NX - k], tab_send.at[k], tab_recv.at[NX - k], x_peer(k))
        for k in range(1, NX)
    ]
    for copy in tab_copies:
        copy.start()
    for slot in range(PEERS - 1, 0, -1):
        id_copies[slot].start()
    for slot in range(PEERS - 1, 0, -1):
        sp_copies[slot].start()

    lane = lax.broadcasted_iota(jnp.int32, (1, 128), 1)
    low_half = lane < 64
    low_half16 = lax.broadcasted_iota(jnp.int32, (16, 128), 1) < 64
    base = group * (NX * ROWS)
    low_rows = lax.broadcasted_iota(jnp.int32, (LOW, WIDE), 0)

    def look_up(chunk, j, rows):
        lhs = jnp.concatenate(
            [tab[j, :, b * LOW : (b + 1) * LOW] for b in range(HIGH)], axis=0
        )
        found = jnp.dot(lhs, hot[chunk], preferred_element_type=jnp.float32)
        high = highs[chunk]
        owner = lax.rem(x + j, NX)
        for b in range(HIGH):
            rows = jnp.where(high == owner * HIGH + b, found[b * F : (b + 1) * F], rows)
        return rows

    for chunk in range(CHUNKS):
        slots = range(chunk * PER, (chunk + 1) * PER)
        for slot in slots:
            if slot:
                id_copies[BACK[slot]].wait_recv()
        lines = [ids[slot : slot + 1, :] for slot in slots]
        wanted = jnp.concatenate(
            [jnp.where(low_half, a, b) for a, b in zip(lines[::2], lines[1::2])], axis=1
        ) - base
        highs[chunk] = wanted >> 8
        hot[chunk] = jnp.where(low_rows == (wanted & (LOW - 1)), 1.0, 0.0).astype(jnp.bfloat16)
        sums[chunk] = look_up(chunk, 0, jnp.zeros((F, WIDE), jnp.float32))

    for slot in range(1, PEERS):
        sp_copies[slot].wait_recv()
    sx_copies = [
        remote(small.at[x], small.at[x], sx_send.at[k], sx_recv.at[NX - k], x_peer(k))
        for k in range(1, NX)
    ]
    for copy in sx_copies:
        copy.start()

    for j in (1, 3):
        tab_copies[NX - j - 1].wait_recv()
        for chunk in range(CHUNKS):
            sums[chunk] = look_up(chunk, j, sums[chunk])
    tab_copies[1].wait_recv()
    row_copies = []
    for chunk in range(CHUNKS - 1, -1, -1):
        rows = look_up(chunk, 2, sums[chunk])
        for half in range(PER // 2):
            part = rows[:, half * 128 : (half + 1) * 128]
            upper, lower = part[:16], part[16:]
            turned_upper = pltpu.roll(upper, 64, 1)
            turned_lower = pltpu.roll(lower, 64, 1)
            even = jnp.where(low_half16, upper, turned_lower).astype(jnp.bfloat16)
            odd = jnp.where(low_half16, turned_upper, lower).astype(jnp.bfloat16)
            slot = chunk * PER + 2 * half
            if slot:
                send[slot] = even
            else:
                recv[0] = even
            send[slot + 1] = odd
        for slot in range((chunk + 1) * PER - 1, max(chunk * PER, 1) - 1, -1):
            copy = remote(
                send.at[slot], recv.at[BACK[slot]], row_send.at[slot],
                row_recv.at[BACK[slot]], plane_peer(slot),
            )
            copy.start()
            row_copies.append(copy)

    for copy in sx_copies:
        copy.wait_recv()
    wanted = sid[...]
    place = ((wanted >> 1) & (NX - 1)) * 64 + (wanted >> 3) * 2 + (wanted & 1)
    small_hot = jnp.where(
        lax.broadcasted_iota(jnp.int32, (256, EX), 0) == place, 1.0, 0.0
    ).astype(jnp.bfloat16)
    small_rows = jnp.concatenate([small[k] for k in range(NX)], axis=0).astype(jnp.bfloat16)
    out_ref[2] = lax.dot_general(
        small_hot, small_rows, (((0,), (0,)), ((), ())), preferred_element_type=jnp.float32
    ).astype(jnp.bfloat16)

    for copy in tab_copies + sx_copies + list(sp_copies.values()) + list(id_copies.values()):
        copy.wait_send()
    for copy in row_copies:
        copy.wait_send()
    for copy in row_copies:
        copy.wait_recv()

    total = recv[0].astype(jnp.float32)
    for slot in range(1, PEERS):
        total = total + recv[slot].astype(jnp.float32)
    both = jnp.concatenate(
        [jnp.where(low_half16, total, 0.0), jnp.where(low_half16, 0.0, total)], axis=0
    ).astype(jnp.bfloat16)
    example = lax.broadcasted_iota(jnp.int32, (EX, 128), 0)
    spot = lax.broadcasted_iota(jnp.int32, (EX, 128), 1)
    picks = jnp.where((spot & (EX - 1)) == example, 1.0, 0.0).astype(jnp.bfloat16)
    pooled = lax.dot_general(
        picks, both, (((1,), (1,)), ((), ())), preferred_element_type=jnp.float32
    )
    out_ref[1] = (pooled * 2 ** (-0.5)).astype(jnp.bfloat16)


def shards(row_numbers, item_table, dense_part, small_ids, small_table):
    dma = pltpu.SemaphoreType.DMA
    parts = pl.pallas_call(
        kernel,
        out_shape=jax.ShapeDtypeStruct((3, EX, F), jnp.bfloat16),
        in_specs=[pl.BlockSpec(memory_space=pltpu.HBM)] * 5,
        out_specs=pl.BlockSpec(memory_space=pltpu.VMEM),
        scratch_shapes=[
            pltpu.VMEM((2, EX), jnp.int32),
            pltpu.VMEM((EX, F), jnp.float32),
            pltpu.VMEM((1, EX), jnp.int32),
            pltpu.VMEM((2, F), jnp.bfloat16),
            pltpu.VMEM((1, 128), jnp.int32),
            pltpu.VMEM((PEERS, 128), jnp.int32),
            pltpu.VMEM((NX, F, ROWS), jnp.bfloat16),
            pltpu.VMEM((CHUNKS, LOW, WIDE), jnp.bfloat16),
            pltpu.VMEM((CHUNKS, 1, WIDE), jnp.int32),
            pltpu.VMEM((CHUNKS, F, WIDE), jnp.float32),
            pltpu.VMEM((PEERS, 16, 128), jnp.bfloat16),
            pltpu.VMEM((PEERS, 16, 128), jnp.bfloat16),
            pltpu.VMEM((NX, 2 * PEERS, F), jnp.float32),
            dma((5,)), dma((NX,)), dma((NX,)), dma((PEERS,)), dma((PEERS,)),
            dma((PEERS,)), dma((PEERS,)), dma((NX,)), dma((NX,)), dma((PEERS,)), dma((PEERS,)),
        ],
        compiler_params=pltpu.CompilerParams(
            collective_id=0, has_side_effects=True, vmem_limit_bytes=16 * 2**20
        ),
    )(*(pltpu.with_memory_space_constraint(a, pltpu.HBM) for a in (row_numbers.T, item_table.T, dense_part, small_ids.reshape(1, EX), small_table)))
    return parts.transpose(1, 0, 2)


def solution(mesh):
    torus = Mesh(mesh.devices.reshape(NZ, NY, NX, 2), (*ROW, "width"))
    return jax.shard_map(
        shards,
        mesh=torus,
        in_specs=(P(ROW, None), P(ROW, "width"), P(ROW, "width"), P(ROW), P(ROW, "width")),
        out_specs=P(ROW, None, "width"),
        check_vma=False,
    )
```

```python
import jax
import jax.numpy as jnp
from jax import lax
from jax.experimental import pallas as pl
from jax.experimental.pallas import tpu as pltpu
from jax.sharding import Mesh
from jax.sharding import PartitionSpec as P

ROW = ("row_0", "row_1", "row_2")
NZ, NY, NX = 8, 4, 4
MESH = pl.DeviceIdType.MESH
BLOCKS = ((0, 0), (1, 0), (0, 1), (0, 3), (1, 1), (1, 3), (0, 2), (1, 2))
FROM = [BLOCKS.index((ky, -kx % NX)) for ky, kx in BLOCKS]
OWNERS = len(BLOCKS)
OFFSETS = sorted(
    ((kz, ky) for kz in range(NZ) for ky in range(2)),
    key=lambda k: (min(k[0], NZ - k[0]) + k[1], k),
)
BACK = [OFFSETS.index((-kz % NZ, ky)) for kz, ky in OFFSETS]
PEERS = len(OFFSETS)
ROWS = 1024
LOW = 256
HIGH = ROWS // LOW
EX = 32
F = 32
CHUNKS = 2
PER = PEERS // CHUNKS
WIDE = PER * 64


def kernel(
    ids_hbm, table_hbm, dense_hbm, sid_hbm, small_hbm, out_ref,
    ids_in, dense, sid, small_in, msg, ids, tab, hot, highs, sums, send, recv, small,
    local_sem, send_sem, tab_sem, ids_sem, row_sem, small_sem, ready,
):
    z, y, x, w = (lax.axis_index(name) for name in (*ROW, "width"))
    odd = lax.rem(y, 2)
    pair_block = z * 2 + y // 2

    def gather_peer(slot, core):
        ky, kx = BLOCKS[slot]
        return (z, y + 1 - 2 * odd if ky else y, lax.rem(x + kx, NX), core)

    def exchange_peer(slot, core):
        kz, ky = OFFSETS[slot]
        return (lax.rem(z + kz, NZ), NY - 1 - y if ky else y, x, core)

    barrier = pltpu.get_barrier_semaphore()
    other = (z, y, x, 1 - w)
    for slot in range(1, OWNERS):
        pl.semaphore_signal(barrier, inc=1, device_id=gather_peer(slot, 0), device_id_type=MESH)
    for slot in range(PEERS - 1, 0, -1):
        pl.semaphore_signal(barrier, inc=1, device_id=exchange_peer(slot, 1), device_id_type=MESH)
    pl.semaphore_signal(barrier, inc=1, device_id=other, device_id_type=MESH)

    fetches = [
        pltpu.make_async_copy(src, dst, local_sem.at[i])
        for i, (src, dst) in enumerate(
            (
                (table_hbm, tab.at[0]), (small_hbm, small_in), (ids_hbm, ids_in),
                (sid_hbm, sid), (dense_hbm, dense),
            )
        )
    ]
    for fetch in fetches:
        fetch.start()

    def push(src, dst, kind, sem, peer):
        pltpu.make_async_remote_copy(
            src_ref=src, dst_ref=dst, send_sem=send_sem.at[kind], recv_sem=sem,
            device_id=peer, device_id_type=MESH,
        ).start()

    def wait(ref, sem):
        pltpu.make_async_copy(ref, ref, sem).wait()

    fetches[1].wait()
    my_two = small.at[pl.ds((pair_block * 8 + odd * NX + x) * 2, 2)]
    my_two[...] = small_in[...].astype(jnp.float32)
    fetches[2].wait()
    pair = ids_in[...]
    line = jnp.concatenate([pair[0:1], pair[1:2], pair[0:1], pair[1:2]], axis=1)
    msg[...] = line
    ids[0:1, :] = line
    fetches[0].wait()
    fetches[3].wait()
    fetches[4].wait()
    out_ref[0] = dense[...].astype(jnp.bfloat16)

    @pl.when(w == 0)
    def _():
        pl.semaphore_wait(barrier, 2 * (OWNERS - 1) + 1)
        pl.semaphore_signal(ready, inc=1, device_id=other, device_id_type=MESH)

    @pl.when(w == 1)
    def _():
        pl.semaphore_wait(ready, 1)

    for slot in range(1, OWNERS):
        push(my_two, my_two, 3, small_sem.at[0], gather_peer(slot, w))
    for slot in range(1, OWNERS):
        push(tab.at[0], tab.at[FROM[slot]], 1, tab_sem.at[FROM[slot] // 4], gather_peer(slot, w))

    @pl.when(w == 1)
    def _():
        pl.semaphore_wait(barrier, 2 * (PEERS - 1) + 1)
        pl.semaphore_signal(ready, inc=1, device_id=other, device_id_type=MESH)

    @pl.when(w == 0)
    def _():
        pl.semaphore_wait(ready, 1)

    for slot in range(PEERS - 1, 0, -1):
        back = BACK[slot]
        push(msg, ids.at[pl.ds(back, 1)], 0, ids_sem.at[back // PER], exchange_peer(slot, w))
    wait(small.at[pl.ds(0, 2 * (OWNERS - 1))], small_sem.at[0])
    my_block = small.at[pl.ds(pl.multiple_of(pair_block * 16, 16), 16)]
    for slot in range(PEERS - 1, 0, -1):
        push(my_block, my_block, 3, small_sem.at[1], exchange_peer(slot, w))

    lane = lax.broadcasted_iota(jnp.int32, (1, 128), 1)
    low_half = lane < 64
    low_half16 = lax.broadcasted_iota(jnp.int32, (16, 128), 1) < 64
    base = pair_block * (OWNERS * ROWS)
    low_rows = lax.broadcasted_iota(jnp.int32, (LOW, WIDE), 0)

    def look_up(chunk, slots, rows):
        lhs = jnp.concatenate(
            [tab[j, :, b * LOW : (b + 1) * LOW] for j in slots for b in range(HIGH)], axis=0
        )
        found = jnp.dot(lhs, hot[chunk], preferred_element_type=jnp.float32)
        high = highs[chunk]
        at = 0
        for j in slots:
            ky, kx = BLOCKS[j]
            owner = (1 - odd if ky else odd) * NX + lax.rem(x + kx, NX)
            for b in range(HIGH):
                rows = jnp.where(high == owner * HIGH + b, found[at : at + F], rows)
                at += F
        return rows

    for chunk in range(CHUNKS):
        first = max(chunk * PER, 1)
        wait(ids.at[pl.ds(first, (chunk + 1) * PER - first)], ids_sem.at[chunk])
        lines = [ids[slot : slot + 1, :] for slot in range(chunk * PER, (chunk + 1) * PER)]
        wanted = jnp.concatenate(
            [jnp.where(low_half, a, b) for a, b in zip(lines[::2], lines[1::2])], axis=1
        ) - base
        highs[chunk] = wanted >> 8
        hot[chunk] = jnp.where(low_rows == (wanted & (LOW - 1)), 1.0, 0.0).astype(jnp.bfloat16)
        if chunk == 0:
            wait(tab.at[pl.ds(1, 3)], tab_sem.at[0])
        sums[chunk] = look_up(chunk, range(4), jnp.zeros((F, WIDE), jnp.float32))

    wait(tab.at[pl.ds(4, 4)], tab_sem.at[1])
    for chunk in range(CHUNKS - 1, -1, -1):
        rows = look_up(chunk, range(4, 8), sums[chunk])
        for half in range(PER // 2):
            part = rows[:, half * 128 : (half + 1) * 128]
            upper, lower = part[:16], part[16:]
            turned_upper = pltpu.roll(upper, 64, 1)
            turned_lower = pltpu.roll(lower, 64, 1)
            slot = chunk * PER + 2 * half
            even = jnp.where(low_half16, upper, turned_lower).astype(jnp.bfloat16)
            if slot:
                send[slot] = even
            else:
                recv[0] = even
            send[slot + 1] = jnp.where(low_half16, turned_upper, lower).astype(jnp.bfloat16)
        for slot in range((chunk + 1) * PER - 1, max(chunk * PER, 1) - 1, -1):
            push(send.at[slot], recv.at[BACK[slot]], 2, row_sem.at[0], exchange_peer(slot, w))

    wait(small.at[pl.ds(0, 16 * (PEERS - 1))], small_sem.at[1])
    small_hot = jnp.where(
        lax.broadcasted_iota(jnp.int32, (256, EX), 0) == sid[...], 1.0, 0.0
    ).astype(jnp.bfloat16)
    out_ref[2] = lax.dot_general(
        small_hot, small[...].astype(jnp.bfloat16), (((0,), (0,)), ((), ())),
        preferred_element_type=jnp.float32,
    ).astype(jnp.bfloat16)

    wait(ids.at[pl.ds(1, PEERS - 1)], send_sem.at[0])
    wait(tab.at[pl.ds(1, OWNERS - 1)], send_sem.at[1])
    wait(small.at[pl.ds(0, 2 * (OWNERS - 1) + 16 * (PEERS - 1))], send_sem.at[3])
    wait(send.at[pl.ds(1, PEERS - 1)], send_sem.at[2])
    wait(recv.at[pl.ds(1, PEERS - 1)], row_sem.at[0])
    total = recv[0].astype(jnp.float32)
    for slot in range(1, PEERS):
        total = total + recv[slot].astype(jnp.float32)
    both = jnp.concatenate(
        [jnp.where(low_half16, total, 0.0), jnp.where(low_half16, 0.0, total)], axis=0
    ).astype(jnp.bfloat16)
    example = lax.broadcasted_iota(jnp.int32, (EX, 128), 0)
    spot = lax.broadcasted_iota(jnp.int32, (EX, 128), 1)
    picks = jnp.where((spot & (EX - 1)) == example, 1.0, 0.0).astype(jnp.bfloat16)
    pooled = lax.dot_general(
        picks, both, (((1,), (1,)), ((), ())), preferred_element_type=jnp.float32
    )
    out_ref[1] = (pooled * 2 ** (-0.5)).astype(jnp.bfloat16)


def shards(row_numbers, item_table, dense_part, small_ids, small_table):
    dma = pltpu.SemaphoreType.DMA
    arrays = row_numbers.T, item_table.T, dense_part, small_ids.reshape(1, EX), small_table
    parts = pl.pallas_call(
        kernel,
        out_shape=jax.ShapeDtypeStruct((3, EX, F), jnp.bfloat16),
        in_specs=[pl.BlockSpec(memory_space=pltpu.HBM)] * 5,
        out_specs=pl.BlockSpec(memory_space=pltpu.VMEM),
        scratch_shapes=[
            pltpu.VMEM((2, EX), jnp.int32),
            pltpu.VMEM((EX, F), jnp.float32),
            pltpu.VMEM((1, EX), jnp.int32),
            pltpu.VMEM((2, F), jnp.bfloat16),
            pltpu.VMEM((1, 128), jnp.int32),
            pltpu.VMEM((PEERS, 128), jnp.int32),
            pltpu.VMEM((OWNERS, F, ROWS), jnp.bfloat16),
            pltpu.VMEM((CHUNKS, LOW, WIDE), jnp.bfloat16),
            pltpu.VMEM((CHUNKS, 1, WIDE), jnp.int32),
            pltpu.VMEM((CHUNKS, F, WIDE), jnp.float32),
            pltpu.VMEM((PEERS, 16, 128), jnp.bfloat16),
            pltpu.VMEM((PEERS, 16, 128), jnp.bfloat16),
            pltpu.VMEM((2 * OWNERS * PEERS, F), jnp.float32),
            dma((5,)), dma((4,)), dma((2,)), dma((CHUNKS,)), dma((1,)), dma((2,)),
            pltpu.SemaphoreType.REGULAR,
        ],
        compiler_params=pltpu.CompilerParams(
            collective_id=0, has_side_effects=True, vmem_limit_bytes=16 * 2**20
        ),
    )(*(pltpu.with_memory_space_constraint(array, pltpu.HBM) for array in arrays))
    return parts.transpose(1, 0, 2)


def solution(mesh):
    torus = Mesh(mesh.devices.reshape(NZ, NY, NX, 2), (*ROW, "width"))
    return jax.shard_map(
        shards,
        mesh=torus,
        in_specs=(P(ROW, None), P(ROW, "width"), P(ROW, "width"), P(ROW), P(ROW, "width")),
        out_specs=P(ROW, None, "width"),
        check_vma=False,
    )
```

```python
import jax
import jax.numpy as jnp
from jax import lax
from jax.experimental import pallas as pl
from jax.experimental.pallas import tpu as pltpu
from jax.sharding import Mesh
from jax.sharding import PartitionSpec as P

ROW = ("row_0", "row_1", "row_2")
NZ, NY, NX = 8, 4, 4
MESH = pl.DeviceIdType.MESH
OWNERS = NX
OFFSETS = sorted(
    ((kz, ky) for kz in range(NZ) for ky in range(NY)),
    key=lambda k: (min(k[0], NZ - k[0]) + min(k[1], NY - k[1]), k),
)
BACK = [OFFSETS.index((-kz % NZ, -ky % NY)) for kz, ky in OFFSETS]
PEERS = len(OFFSETS)
ROWS = 1024
LOW = 256
HIGH = ROWS // LOW
EX = 32
F = 32
CHUNKS = 4
PER = PEERS // CHUNKS
WIDE = PER * 64


def kernel(
    ids_hbm, table_hbm, dense_hbm, sid_hbm, small_hbm, out_ref,
    ids_in, dense, sid, small_in, msg, ids, tab, send, recv, small,
    local_sem, send_sem, tab_sem, ids_sem, row_sem, small_sem, ready,
):
    z, y, x, w = (lax.axis_index(name) for name in (*ROW, "width"))
    block = z * NY + y

    def gather_peer(slot, core):
        return (z, y, lax.rem(x + slot, NX), core)

    def exchange_peer(slot, core):
        kz, ky = OFFSETS[slot]
        return (lax.rem(z + kz, NZ), lax.rem(y + ky, NY), x, core)

    barrier = pltpu.get_barrier_semaphore()
    other = (z, y, x, 1 - w)
    for slot in range(1, OWNERS):
        pl.semaphore_signal(barrier, inc=1, device_id=gather_peer(slot, 0), device_id_type=MESH)
    for slot in range(PEERS - 1, 0, -1):
        pl.semaphore_signal(barrier, inc=1, device_id=exchange_peer(slot, 1), device_id_type=MESH)
    pl.semaphore_signal(barrier, inc=1, device_id=other, device_id_type=MESH)

    fetches = [
        pltpu.make_async_copy(src, dst, local_sem.at[i])
        for i, (src, dst) in enumerate(
            (
                (table_hbm, tab.at[0]), (small_hbm, small_in), (ids_hbm, ids_in),
                (sid_hbm, sid), (dense_hbm, dense),
            )
        )
    ]
    for fetch in fetches:
        fetch.start()

    def push(src, dst, kind, sem, peer):
        pltpu.make_async_remote_copy(
            src_ref=src, dst_ref=dst, send_sem=send_sem.at[kind], recv_sem=sem,
            device_id=peer, device_id_type=MESH,
        ).start()

    def wait(ref, sem):
        pltpu.make_async_copy(ref, ref, sem).wait()

    fetches[1].wait()
    two = small_in[...].astype(jnp.float32)
    my_line = small.at[pl.ds(block * NX + x, 1)]
    my_line[...] = jnp.concatenate([two[0:1], two[1:2], two[0:1], two[1:2]], axis=1)
    fetches[2].wait()
    pair = ids_in[...]
    line = jnp.concatenate([pair[0:1], pair[1:2], pair[0:1], pair[1:2]], axis=1)
    msg[...] = line
    ids[0:1, :] = line
    fetches[0].wait()
    fetches[3].wait()
    fetches[4].wait()
    out_ref[0] = dense[...].astype(jnp.bfloat16)

    @pl.when(w == 0)
    def _():
        pl.semaphore_wait(barrier, 2 * (OWNERS - 1) + 1)
        pl.semaphore_signal(ready, inc=1, device_id=other, device_id_type=MESH)

    @pl.when(w == 1)
    def _():
        pl.semaphore_wait(ready, 1)

    for slot in range(1, OWNERS):
        push(my_line, my_line, 3, small_sem.at[0], gather_peer(slot, w))
    for slot in range(OWNERS - 1, 0, -1):
        push(tab.at[0], tab.at[NX - slot], 1, tab_sem.at[0], gather_peer(slot, w))

    @pl.when(w == 1)
    def _():
        pl.semaphore_wait(barrier, 2 * (PEERS - 1) + 1)
        for slot in range(PEERS - 1, 0, -1):
            back = BACK[slot]
            for core in (1, 0):
                push(
                    msg, ids.at[pl.ds(back, 1)], 0, ids_sem.at[back // PER],
                    exchange_peer(slot, core),
                )
        pl.semaphore_signal(ready, inc=1, device_id=other, device_id_type=MESH)

    @pl.when(w == 0)
    def _():
        pl.semaphore_wait(ready, 1)

    wait(small.at[pl.ds(0, OWNERS - 1)], small_sem.at[0])
    my_block = small.at[pl.ds(block * OWNERS, OWNERS)]
    for slot in range(PEERS - 1, 0, -1):
        push(my_block, my_block, 3, small_sem.at[1], exchange_peer(slot, w))

    lane = lax.broadcasted_iota(jnp.int32, (1, 128), 1)
    low_half = lane < 64
    low_half16 = lax.broadcasted_iota(jnp.int32, (16, 128), 1) < 64
    low_rows = lax.broadcasted_iota(jnp.int32, (LOW, WIDE), 0)

    for chunk in range(CHUNKS):
        first = max(chunk * PER, 1)
        slots = range((chunk + 1) * PER - 1, first - 1, -1)
        wait(ids.at[pl.ds(first, len(slots))], ids_sem.at[chunk])
        lines = [ids[slot : slot + 1, :] for slot in range(chunk * PER, (chunk + 1) * PER)]
        wanted = jnp.concatenate(
            [jnp.where(low_half, a, b) for a, b in zip(lines[::2], lines[1::2])], axis=1
        )
        high = wanted >> 8
        hot = jnp.where(low_rows == (wanted & (LOW - 1)), 1.0, 0.0).astype(jnp.bfloat16)
        if chunk == 0:
            wait(tab.at[pl.ds(1, OWNERS - 1)], tab_sem.at[0])
        lhs = jnp.concatenate(
            [tab[j, :, b * LOW : (b + 1) * LOW] for j in range(OWNERS) for b in range(HIGH)], axis=0
        )
        found = jnp.dot(lhs, hot, preferred_element_type=jnp.float32)
        rows = jnp.zeros((F, WIDE), jnp.float32)
        for j in range(OWNERS):
            owner = block * NX + lax.rem(x + j, NX)
            for b in range(HIGH):
                at = (j * HIGH + b) * F
                here = owner * HIGH + b
                rows = jnp.where(high == here, found[at : at + F], rows)
        for half in range(PER // 2):
            part = rows[:, half * 128 : (half + 1) * 128]
            upper, lower = part[:16], part[16:]
            turned_upper = pltpu.roll(upper, 64, 1)
            turned_lower = pltpu.roll(lower, 64, 1)
            slot = chunk * PER + 2 * half
            even = jnp.where(low_half16, upper, turned_lower).astype(jnp.bfloat16)
            if slot:
                send[slot] = even
            else:
                recv[0] = even
            send[slot + 1] = jnp.where(low_half16, turned_upper, lower).astype(jnp.bfloat16)
        for slot in slots:
            push(send.at[slot], recv.at[BACK[slot]], 2, row_sem.at[0], exchange_peer(slot, w))

    wait(small.at[pl.ds(0, OWNERS * (PEERS - 1))], small_sem.at[1])
    wanted = sid[...]
    lines = small[...].astype(jnp.bfloat16)
    small_rows = jnp.zeros((EX, F), jnp.float32)
    for row in range(2):
        spot = jnp.where((wanted & 1) == row, wanted >> 1, -1)
        small_hot = jnp.where(
            lax.broadcasted_iota(jnp.int32, (OWNERS * PEERS, EX), 0) == spot, 1.0, 0.0
        ).astype(jnp.bfloat16)
        small_rows = small_rows + lax.dot_general(
            small_hot, lines[:, row * F : (row + 1) * F], (((0,), (0,)), ((), ())),
            preferred_element_type=jnp.float32,
        )
    out_ref[2] = small_rows.astype(jnp.bfloat16)

    @pl.when(w == 1)
    def _():
        for _ in range(2):
            wait(ids.at[pl.ds(1, PEERS - 1)], send_sem.at[0])

    wait(tab.at[pl.ds(1, OWNERS - 1)], send_sem.at[1])
    wait(small.at[pl.ds(0, OWNERS * PEERS - 1)], send_sem.at[3])
    wait(send.at[pl.ds(1, PEERS - 1)], send_sem.at[2])
    wait(recv.at[pl.ds(1, PEERS - 1)], row_sem.at[0])
    total = recv[0].astype(jnp.float32)
    for slot in range(1, PEERS):
        total = total + recv[slot].astype(jnp.float32)
    both = jnp.concatenate(
        [jnp.where(low_half16, total, 0.0), jnp.where(low_half16, 0.0, total)], axis=0
    ).astype(jnp.bfloat16)
    example = lax.broadcasted_iota(jnp.int32, (EX, 128), 0)
    spot = lax.broadcasted_iota(jnp.int32, (EX, 128), 1)
    picks = jnp.where((spot & (EX - 1)) == example, 1.0, 0.0).astype(jnp.bfloat16)
    pooled = lax.dot_general(
        picks, both, (((1,), (1,)), ((), ())), preferred_element_type=jnp.float32
    )
    out_ref[1] = (pooled * 2 ** (-0.5)).astype(jnp.bfloat16)


def shards(row_numbers, item_table, dense_part, small_ids, small_table):
    dma = pltpu.SemaphoreType.DMA
    arrays = row_numbers.T, item_table.T, dense_part, small_ids.reshape(1, EX), small_table
    parts = pl.pallas_call(
        kernel,
        out_shape=jax.ShapeDtypeStruct((3, EX, F), jnp.bfloat16),
        in_specs=[pl.BlockSpec(memory_space=pltpu.HBM)] * 5,
        out_specs=pl.BlockSpec(memory_space=pltpu.VMEM),
        scratch_shapes=[
            pltpu.VMEM((2, EX), jnp.int32),
            pltpu.VMEM((EX, F), jnp.float32),
            pltpu.VMEM((1, EX), jnp.int32),
            pltpu.VMEM((2, F), jnp.bfloat16),
            pltpu.VMEM((1, 128), jnp.int32),
            pltpu.VMEM((PEERS, 128), jnp.int32),
            pltpu.VMEM((OWNERS, F, ROWS), jnp.bfloat16),
            pltpu.VMEM((PEERS, 16, 128), jnp.bfloat16),
            pltpu.VMEM((PEERS, 16, 128), jnp.bfloat16),
            pltpu.VMEM((OWNERS * PEERS, 128), jnp.float32),
            dma((5,)), dma((4,)), dma((1,)), dma((CHUNKS,)), dma((1,)), dma((2,)),
            pltpu.SemaphoreType.REGULAR,
        ],
        compiler_params=pltpu.CompilerParams(
            collective_id=0, has_side_effects=True, vmem_limit_bytes=16 * 2**20
        ),
    )(*(pltpu.with_memory_space_constraint(array, pltpu.HBM) for array in arrays))
    return parts.transpose(1, 0, 2)


def solution(mesh):
    torus = Mesh(mesh.devices.reshape(NZ, NY, NX, 2), (*ROW, "width"))
    return jax.shard_map(
        shards,
        mesh=torus,
        in_specs=(P(ROW, None), P(ROW, "width"), P(ROW, "width"), P(ROW), P(ROW, "width")),
        out_specs=P(ROW, None, "width"),
        check_vma=False,
    )
```

```python
import jax
import jax.numpy as jnp
from jax import lax
from jax.experimental import pallas as pl
from jax.experimental.pallas import tpu as pltpu
from jax.sharding import Mesh
from jax.sharding import PartitionSpec as P

ROW = ("row_0", "row_1", "row_2")
NZ, NY, NX = 8, 4, 4
MESH = pl.DeviceIdType.MESH
OWNERS = NX
PEERS = NZ * NY
FAR_Z = (4, 3, 5, 2, 6, 1, 7, 0)
FAR_Y = (2, 1, 3, 0)
ROWS = 1024
LOW = 256
HIGH = ROWS // LOW
EX = 32
F = 32
CHUNKS = 8
PLANES = NZ // CHUNKS
PER = PLANES * NY
WIDE = PER * 64


def kernel(
    ids_hbm, table_hbm, dense_hbm, sid_hbm, small_hbm, out_ref,
    ids_in, dense, sid, small_in, msg, ids, tab, send, recv, small,
    local_sem, send_sem, tab_sem, ids_sem, row_sem, small_sem, ready,
):
    z, y, x, w = (lax.axis_index(name) for name in (*ROW, "width"))
    block = z * NY + y

    def gather_peer(slot, core):
        return (z, y, lax.rem(x + slot, NX), core)

    def exchange_peer(plane, ky, core):
        return (plane, lax.rem(y + ky, NY), x, core)

    def my_slot(ky):
        return z * NY + -ky % NY

    barrier = pltpu.get_barrier_semaphore()
    other = (z, y, x, 1 - w)
    for slot in range(1, OWNERS):
        pl.semaphore_signal(barrier, inc=1, device_id=gather_peer(slot, 0), device_id_type=MESH)
    others = [(kz, ky) for kz in FAR_Z for ky in FAR_Y if kz or ky]
    for kz, ky in others:
        peer = exchange_peer(lax.rem(z + kz, NZ), ky, 1)
        pl.semaphore_signal(barrier, inc=1, device_id=peer, device_id_type=MESH)
    pl.semaphore_signal(barrier, inc=1, device_id=other, device_id_type=MESH)

    fetches = [
        pltpu.make_async_copy(src, dst, local_sem.at[i])
        for i, (src, dst) in enumerate(
            (
                (table_hbm, tab.at[0]), (small_hbm, small_in), (ids_hbm, ids_in),
                (sid_hbm, sid), (dense_hbm, dense),
            )
        )
    ]
    for fetch in fetches:
        fetch.start()

    def push(src, dst, kind, sem, peer):
        pltpu.make_async_remote_copy(
            src_ref=src, dst_ref=dst, send_sem=send_sem.at[kind], recv_sem=sem,
            device_id=peer, device_id_type=MESH,
        ).start()

    def wait(ref, sem):
        pltpu.make_async_copy(ref, ref, sem).wait()

    fetches[1].wait()
    two = small_in[...].astype(jnp.float32)
    my_line = small.at[pl.ds(block * NX + x, 1)]
    my_line[...] = jnp.concatenate([two[0:1], two[1:2], two[0:1], two[1:2]], axis=1)
    fetches[2].wait()
    pair = ids_in[...]
    line = jnp.concatenate([pair[0:1], pair[1:2], pair[0:1], pair[1:2]], axis=1)
    msg[...] = line
    pltpu.make_async_copy(msg, ids.at[pl.ds(my_slot(0), 1)], ids_sem.at[z // PLANES]).start()
    fetches[0].wait()
    fetches[3].wait()
    fetches[4].wait()
    out_ref[0] = dense[...].astype(jnp.bfloat16)

    @pl.when(w == 0)
    def _():
        pl.semaphore_wait(barrier, 2 * (OWNERS - 1) + 1)
        pl.semaphore_signal(ready, inc=1, device_id=other, device_id_type=MESH)

    @pl.when(w == 1)
    def _():
        pl.semaphore_wait(ready, 1)

    for slot in range(1, OWNERS):
        push(my_line, my_line, 3, small_sem.at[0], gather_peer(slot, w))
    for slot in range(OWNERS - 1, 0, -1):
        push(tab.at[0], tab.at[NX - slot], 1, tab_sem.at[0], gather_peer(slot, w))

    @pl.when(w == 1)
    def _():
        pl.semaphore_wait(barrier, 2 * (PEERS - 1) + 1)
        for kz, ky in others:
            for core in (1, 0):
                push(
                    msg, ids.at[pl.ds(my_slot(ky), 1)], 0, ids_sem.at[z // PLANES],
                    exchange_peer(lax.rem(z + kz, NZ), ky, core),
                )
        pl.semaphore_signal(ready, inc=1, device_id=other, device_id_type=MESH)

    @pl.when(w == 0)
    def _():
        pl.semaphore_wait(ready, 1)

    wait(small.at[pl.ds(0, OWNERS - 1)], small_sem.at[0])
    my_block = small.at[pl.ds(block * OWNERS, OWNERS)]
    for kz, ky in others:
        push(my_block, my_block, 3, small_sem.at[1], exchange_peer(lax.rem(z + kz, NZ), ky, w))

    lane = lax.broadcasted_iota(jnp.int32, (1, 128), 1)
    low_half = lane < 64
    low_half16 = lax.broadcasted_iota(jnp.int32, (16, 128), 1) < 64
    low_rows = lax.broadcasted_iota(jnp.int32, (LOW, WIDE), 0)

    for chunk in range(CHUNKS):
        wait(ids.at[pl.ds(chunk * PER, PER)], ids_sem.at[chunk])
        lines = [ids[slot : slot + 1, :] for slot in range(chunk * PER, (chunk + 1) * PER)]
        wanted = jnp.concatenate(
            [jnp.where(low_half, a, b) for a, b in zip(lines[::2], lines[1::2])], axis=1
        )
        high = wanted >> 8
        hot = jnp.where(low_rows == (wanted & (LOW - 1)), 1.0, 0.0).astype(jnp.bfloat16)
        if chunk == 0:
            wait(tab.at[pl.ds(1, OWNERS - 1)], tab_sem.at[0])
        lhs = jnp.concatenate(
            [tab[j, :, b * LOW : (b + 1) * LOW] for j in range(OWNERS) for b in range(HIGH)], axis=0
        )
        found = jnp.dot(lhs, hot, preferred_element_type=jnp.float32)
        rows = jnp.zeros((F, WIDE), jnp.float32)
        for j in range(OWNERS):
            owner = block * NX + lax.rem(x + j, NX)
            for b in range(HIGH):
                at = (j * HIGH + b) * F
                here = owner * HIGH + b
                rows = jnp.where(high == here, found[at : at + F], rows)
        for half in range(PER // 2):
            part = rows[:, half * 128 : (half + 1) * 128]
            upper, lower = part[:16], part[16:]
            turned_upper = pltpu.roll(upper, 64, 1)
            turned_lower = pltpu.roll(lower, 64, 1)
            slot = chunk * PER + 2 * half
            send[slot] = jnp.where(low_half16, upper, turned_lower).astype(jnp.bfloat16)
            send[slot + 1] = jnp.where(low_half16, turned_upper, lower).astype(jnp.bfloat16)
        for plane in range(chunk * PLANES, (chunk + 1) * PLANES):
            for ky in FAR_Y:
                source, target = send.at[plane * NY + ky], recv.at[my_slot(ky)]
                if ky:
                    push(source, target, 2, row_sem.at[0], exchange_peer(plane, ky, w))
                    continue

                @pl.when(plane != z)
                def _():
                    push(source, target, 2, row_sem.at[0], exchange_peer(plane, ky, w))

                @pl.when(plane == z)
                def _():
                    pltpu.make_async_copy(source, target, row_sem.at[0]).start()

    wait(small.at[pl.ds(0, OWNERS * (PEERS - 1))], small_sem.at[1])
    wanted = sid[...]
    lines = small[...].astype(jnp.bfloat16)
    small_rows = jnp.zeros((EX, F), jnp.float32)
    for row in range(2):
        spot = jnp.where((wanted & 1) == row, wanted >> 1, -1)
        small_hot = jnp.where(
            lax.broadcasted_iota(jnp.int32, (OWNERS * PEERS, EX), 0) == spot, 1.0, 0.0
        ).astype(jnp.bfloat16)
        small_rows = small_rows + lax.dot_general(
            small_hot, lines[:, row * F : (row + 1) * F], (((0,), (0,)), ((), ())),
            preferred_element_type=jnp.float32,
        )
    out_ref[2] = small_rows.astype(jnp.bfloat16)

    @pl.when(w == 1)
    def _():
        for _ in range(2):
            wait(ids.at[pl.ds(1, PEERS - 1)], send_sem.at[0])

    wait(tab.at[pl.ds(1, OWNERS - 1)], send_sem.at[1])
    wait(small.at[pl.ds(0, OWNERS * PEERS - 1)], send_sem.at[3])
    wait(send.at[pl.ds(1, PEERS - 1)], send_sem.at[2])
    wait(recv.at[pl.ds(0, PEERS)], row_sem.at[0])
    total = recv[0].astype(jnp.float32)
    for slot in range(1, PEERS):
        total = total + recv[slot].astype(jnp.float32)
    both = jnp.concatenate(
        [jnp.where(low_half16, total, 0.0), jnp.where(low_half16, 0.0, total)], axis=0
    ).astype(jnp.bfloat16)
    example = lax.broadcasted_iota(jnp.int32, (EX, 128), 0)
    spot = lax.broadcasted_iota(jnp.int32, (EX, 128), 1)
    picks = jnp.where((spot & (EX - 1)) == example, 1.0, 0.0).astype(jnp.bfloat16)
    pooled = lax.dot_general(
        picks, both, (((1,), (1,)), ((), ())), preferred_element_type=jnp.float32
    )
    out_ref[1] = (pooled * 2 ** (-0.5)).astype(jnp.bfloat16)


def shards(row_numbers, item_table, dense_part, small_ids, small_table):
    dma = pltpu.SemaphoreType.DMA
    arrays = row_numbers.T, item_table.T, dense_part, small_ids.reshape(1, EX), small_table
    parts = pl.pallas_call(
        kernel,
        out_shape=jax.ShapeDtypeStruct((3, EX, F), jnp.bfloat16),
        in_specs=[pl.BlockSpec(memory_space=pltpu.HBM)] * 5,
        out_specs=pl.BlockSpec(memory_space=pltpu.VMEM),
        scratch_shapes=[
            pltpu.VMEM((2, EX), jnp.int32),
            pltpu.VMEM((EX, F), jnp.float32),
            pltpu.VMEM((1, EX), jnp.int32),
            pltpu.VMEM((2, F), jnp.bfloat16),
            pltpu.VMEM((1, 128), jnp.int32),
            pltpu.VMEM((PEERS, 128), jnp.int32),
            pltpu.VMEM((OWNERS, F, ROWS), jnp.bfloat16),
            pltpu.VMEM((PEERS, 16, 128), jnp.bfloat16),
            pltpu.VMEM((PEERS, 16, 128), jnp.bfloat16),
            pltpu.VMEM((OWNERS * PEERS, 128), jnp.float32),
            dma((5,)), dma((4,)), dma((1,)), dma((CHUNKS,)), dma((1,)), dma((2,)),
            pltpu.SemaphoreType.REGULAR,
        ],
        compiler_params=pltpu.CompilerParams(
            collective_id=0, has_side_effects=True, vmem_limit_bytes=16 * 2**20
        ),
    )(*(pltpu.with_memory_space_constraint(array, pltpu.HBM) for array in arrays))
    return parts.transpose(1, 0, 2)


def solution(mesh):
    torus = Mesh(mesh.devices.reshape(NZ, NY, NX, 2), (*ROW, "width"))
    return jax.shard_map(
        shards,
        mesh=torus,
        in_specs=(P(ROW, None), P(ROW, "width"), P(ROW, "width"), P(ROW), P(ROW, "width")),
        out_specs=P(ROW, None, "width"),
        check_vma=False,
    )
```

```python
import jax
import jax.numpy as jnp
from jax import lax
from jax.experimental import pallas as pl
from jax.experimental.pallas import tpu as pltpu
from jax.sharding import Mesh
from jax.sharding import PartitionSpec as P

ROW = ("row_0", "row_1", "row_2")
NZ, NY, NX = 8, 4, 4
MESH = pl.DeviceIdType.MESH
BLOCKS = ((0, 0), (0, 1), (1, 0), (1, 1))
OWNERS = len(BLOCKS)
SIDES = len(BLOCKS)
PEERS = NZ * SIDES
FAR_Z = (4, 3, 5, 2, 6, 1, 7)
FAR_SIDE = (3, 1, 2, 0)
ROWS = 1024
LOW = 256
HIGH = ROWS // LOW
EX = 32
F = 32
WIDE = SIDES * 64


def kernel(
    ids_hbm, table_hbm, dense_hbm, sid_hbm, small_hbm, out_ref,
    ids_in, dense, sid, small_in, ring, ids, tab, send, recv, small,
    local_sem, send_sem, tab_sem, ring_sem, ids_sem, row_sem, small_sem, ready,
):
    z, y, x, w = (lax.axis_index(name) for name in (*ROW, "width"))
    odd_y, odd_x = lax.rem(y, 2), lax.rem(x, 2)
    half_y, half_x = y // 2, x // 2
    quarter = half_y * 2 + half_x
    block = z * SIDES + quarter

    def owner(slot):
        fy, fx = BLOCKS[slot]
        return y + 1 - 2 * odd_y if fy else y, x + 1 - 2 * odd_x if fx else x

    def gather_peer(slot, core):
        return (z, *owner(slot), core)

    def mirror_peer(plane, side, core):
        my, mx = BLOCKS[side]
        return (plane, NY - 1 - y if my else y, NX - 1 - x if mx else x, core)

    def mirror_line(side):
        my, mx = BLOCKS[side]
        return (1 - half_y if my else half_y) * 2 + (1 - half_x if mx else half_x)

    def z_peer(kz, core):
        return (lax.rem(z + kz, NZ), y, x, core)

    barrier = pltpu.get_barrier_semaphore()
    other = (z, y, x, 1 - w)
    for kz in FAR_Z:
        pl.semaphore_signal(barrier, inc=1, device_id=z_peer(kz, 1), device_id_type=MESH)
    for slot in range(1, OWNERS):
        pl.semaphore_signal(barrier, inc=1, device_id=gather_peer(slot, 0), device_id_type=MESH)
    pl.semaphore_signal(barrier, inc=1, device_id=other, device_id_type=MESH)

    @pl.when(w == 1)
    def _():
        for side in range(1, SIDES):
            peer = mirror_peer(z, side, 0)
            pl.semaphore_signal(barrier, inc=1, device_id=peer, device_id_type=MESH)


    fetches = [
        pltpu.make_async_copy(src, dst, local_sem.at[i])
        for i, (src, dst) in enumerate(
            (
                (table_hbm, tab.at[0]), (small_hbm, small_in), (ids_hbm, ids_in),
                (sid_hbm, sid), (dense_hbm, dense),
            )
        )
    ]
    for fetch in fetches:
        fetch.start()

    def push(src, dst, kind, sem, peer):
        pltpu.make_async_remote_copy(
            src_ref=src, dst_ref=dst, send_sem=send_sem.at[kind], recv_sem=sem,
            device_id=peer, device_id_type=MESH,
        ).start()

    def wait(ref, sem):
        pltpu.make_async_copy(ref, ref, sem).wait()

    fetches[1].wait()
    two = small_in[...].astype(jnp.float32)
    my_line = small.at[pl.ds(block * OWNERS + odd_y * 2 + odd_x, 1)]
    my_line[...] = jnp.concatenate([two[0:1], two[1:2], two[0:1], two[1:2]], axis=1)
    fetches[2].wait()
    pair = ids_in[...]
    line = jnp.concatenate([pair[0:1], pair[1:2], pair[0:1], pair[1:2]], axis=1)
    my_ring = ring.at[pl.ds(quarter, 1)]
    my_ring[...] = line
    fetches[0].wait()
    fetches[3].wait()
    fetches[4].wait()
    out_ref[0] = dense[...].astype(jnp.bfloat16)

    @pl.when(w == 0)
    def _():
        pl.semaphore_wait(barrier, 2 * (OWNERS - 1) + SIDES)
        pl.semaphore_signal(ready, inc=1, device_id=other, device_id_type=MESH)

    @pl.when(w == 1)
    def _():
        pl.semaphore_wait(ready, 1)
        for side in FAR_SIDE[:-1]:
            push(my_ring, my_ring, 0, ring_sem.at[0], mirror_peer(z, side, 1))

    for slot in range(1, OWNERS):
        push(my_line, my_line, 3, small_sem.at[0], gather_peer(slot, w))
    for slot in range(OWNERS - 1, 0, -1):
        push(tab.at[0], tab.at[slot], 1, tab_sem.at[0], gather_peer(slot, w))

    @pl.when(w == 1)
    def _():
        bundle = ids.at[pl.ds(z * SIDES, SIDES)]
        pl.semaphore_wait(barrier, 2 * (NZ - 1) + 1)
        wait(ring.at[pl.ds(0, SIDES - 1)], ring_sem.at[0])
        for kz in FAR_Z:
            for core in (1, 0):
                push(ring, bundle, 0, ids_sem.at[z], z_peer(kz, core))
        push(ring, bundle, 0, ids_sem.at[z], other)
        pltpu.make_async_copy(ring, bundle, ids_sem.at[z]).start()

    wait(small.at[pl.ds(0, OWNERS - 1)], small_sem.at[0])
    my_block = small.at[pl.ds(block * OWNERS, OWNERS)]

    lane = lax.broadcasted_iota(jnp.int32, (1, 128), 1)
    low_half = lane < 64
    low_half16 = lax.broadcasted_iota(jnp.int32, (16, 128), 1) < 64
    low_rows = lax.broadcasted_iota(jnp.int32, (LOW, WIDE), 0)

    for plane in range(NZ):
        wait(ids.at[pl.ds(plane * SIDES, SIDES)], ids_sem.at[plane])
        for side in FAR_SIDE:
            if side:
                push(my_block, my_block, 3, small_sem.at[1], mirror_peer(plane, side, w))
                continue

            @pl.when(plane != z)
            def _():
                push(my_block, my_block, 3, small_sem.at[1], mirror_peer(plane, side, w))

        lines = [ids[pl.ds(plane * SIDES + mirror_line(side), 1), :] for side in range(SIDES)]
        wanted = jnp.concatenate(
            [jnp.where(low_half, a, b) for a, b in zip(lines[::2], lines[1::2])], axis=1
        )
        high = wanted >> 8
        hot = jnp.where(low_rows == (wanted & (LOW - 1)), 1.0, 0.0).astype(jnp.bfloat16)
        if plane == 0:
            wait(tab.at[pl.ds(1, OWNERS - 1)], tab_sem.at[0])
        lhs = jnp.concatenate(
            [tab[j, :, b * LOW : (b + 1) * LOW] for j in range(OWNERS) for b in range(HIGH)], axis=0
        )
        found = jnp.dot(lhs, hot, preferred_element_type=jnp.float32)
        rows = jnp.zeros((F, WIDE), jnp.float32)
        for j in range(OWNERS):
            yo, xo = owner(j)
            for b in range(HIGH):
                at = (j * HIGH + b) * F
                here = ((z * NY + yo) * NX + xo) * HIGH + b
                rows = jnp.where(high == here, found[at : at + F], rows)
        for half in range(SIDES // 2):
            part = rows[:, half * 128 : (half + 1) * 128]
            upper, lower = part[:16], part[16:]
            turned_upper = pltpu.roll(upper, 64, 1)
            turned_lower = pltpu.roll(lower, 64, 1)
            slot = plane * SIDES + 2 * half
            send[slot] = jnp.where(low_half16, upper, turned_lower).astype(jnp.bfloat16)
            send[slot + 1] = jnp.where(low_half16, turned_upper, lower).astype(jnp.bfloat16)
        for side in FAR_SIDE:
            source, target = send.at[plane * SIDES + side], recv.at[block]
            if side:
                push(source, target, 2, row_sem.at[0], mirror_peer(plane, side, w))
                continue

            @pl.when(plane != z)
            def _():
                push(source, target, 2, row_sem.at[0], mirror_peer(plane, side, w))

            @pl.when(plane == z)
            def _():
                pltpu.make_async_copy(source, target, row_sem.at[0]).start()

    wait(small.at[pl.ds(0, OWNERS * (PEERS - 1))], small_sem.at[1])
    wanted = sid[...]
    device = wanted >> 1
    line = (device & 0x79) | ((device & 2) << 1) | ((device & 4) >> 1)
    lines = small[...].astype(jnp.bfloat16)
    small_rows = jnp.zeros((EX, F), jnp.float32)
    for row in range(2):
        spot = jnp.where((wanted & 1) == row, line, -1)
        small_hot = jnp.where(
            lax.broadcasted_iota(jnp.int32, (OWNERS * PEERS, EX), 0) == spot, 1.0, 0.0
        ).astype(jnp.bfloat16)
        small_rows = small_rows + lax.dot_general(
            small_hot, lines[:, row * F : (row + 1) * F], (((0,), (0,)), ((), ())),
            preferred_element_type=jnp.float32,
        )
    out_ref[2] = small_rows.astype(jnp.bfloat16)

    @pl.when(w == 1)
    def _():
        wait(ids.at[pl.ds(0, PEERS)], send_sem.at[0])
        wait(ids.at[pl.ds(0, PEERS - 1)], send_sem.at[0])

    wait(tab.at[pl.ds(1, OWNERS - 1)], send_sem.at[1])
    wait(small.at[pl.ds(0, OWNERS * PEERS - 1)], send_sem.at[3])
    wait(send.at[pl.ds(1, PEERS - 1)], send_sem.at[2])
    wait(recv.at[pl.ds(0, PEERS)], row_sem.at[0])
    total = recv[0].astype(jnp.float32)
    for slot in range(1, PEERS):
        total = total + recv[slot].astype(jnp.float32)
    both = jnp.concatenate(
        [jnp.where(low_half16, total, 0.0), jnp.where(low_half16, 0.0, total)], axis=0
    ).astype(jnp.bfloat16)
    example = lax.broadcasted_iota(jnp.int32, (EX, 128), 0)
    spot = lax.broadcasted_iota(jnp.int32, (EX, 128), 1)
    picks = jnp.where((spot & (EX - 1)) == example, 1.0, 0.0).astype(jnp.bfloat16)
    pooled = lax.dot_general(
        picks, both, (((1,), (1,)), ((), ())), preferred_element_type=jnp.float32
    )
    out_ref[1] = (pooled * 2 ** (-0.5)).astype(jnp.bfloat16)


def shards(row_numbers, item_table, dense_part, small_ids, small_table):
    dma = pltpu.SemaphoreType.DMA
    arrays = row_numbers.T, item_table.T, dense_part, small_ids.reshape(1, EX), small_table
    parts = pl.pallas_call(
        kernel,
        out_shape=jax.ShapeDtypeStruct((3, EX, F), jnp.bfloat16),
        in_specs=[pl.BlockSpec(memory_space=pltpu.HBM)] * 5,
        out_specs=pl.BlockSpec(memory_space=pltpu.VMEM),
        scratch_shapes=[
            pltpu.VMEM((2, EX), jnp.int32),
            pltpu.VMEM((EX, F), jnp.float32),
            pltpu.VMEM((1, EX), jnp.int32),
            pltpu.VMEM((2, F), jnp.bfloat16),
            pltpu.VMEM((SIDES, 128), jnp.int32),
            pltpu.VMEM((PEERS, 128), jnp.int32),
            pltpu.VMEM((OWNERS, F, ROWS), jnp.bfloat16),
            pltpu.VMEM((PEERS, 16, 128), jnp.bfloat16),
            pltpu.VMEM((PEERS, 16, 128), jnp.bfloat16),
            pltpu.VMEM((OWNERS * PEERS, 128), jnp.float32),
            dma((5,)), dma((4,)), dma((1,)), dma((1,)), dma((NZ,)), dma((1,)), dma((2,)),
            pltpu.SemaphoreType.REGULAR,
        ],
        compiler_params=pltpu.CompilerParams(
            collective_id=0, has_side_effects=True, vmem_limit_bytes=16 * 2**20
        ),
    )(*(pltpu.with_memory_space_constraint(array, pltpu.HBM) for array in arrays))
    return parts.transpose(1, 0, 2)


def solution(mesh):
    torus = Mesh(mesh.devices.reshape(NZ, NY, NX, 2), (*ROW, "width"))
    return jax.shard_map(
        shards,
        mesh=torus,
        in_specs=(P(ROW, None), P(ROW, "width"), P(ROW, "width"), P(ROW), P(ROW, "width")),
        out_specs=P(ROW, None, "width"),
        check_vma=False,
    )
```

```python
import jax
import jax.numpy as jnp
from jax import lax
from jax.experimental import pallas as pl
from jax.experimental.pallas import tpu as pltpu
from jax.sharding import Mesh
from jax.sharding import PartitionSpec as P

ROW = ("row_0", "row_1", "row_2")
NZ, NY, NX = 8, 4, 4
MESH = pl.DeviceIdType.MESH
BLOCKS = ((0, 0), (0, 1), (1, 0), (1, 1))
OWNERS = len(BLOCKS)
SIDES = len(BLOCKS)
PEERS = NZ * SIDES
FAR_Z = (4, 3, 5, 2, 6, 1, 7)
FAR_SIDE = (3, 1, 2, 0)
ROWS = 1024
LOW = 256
HIGH = ROWS // LOW
EX = 32
F = 32
WIDE = SIDES * 64


def kernel(
    ids_hbm, table_hbm, dense_hbm, sid_hbm, small_hbm, out_ref,
    ids_in, dense, sid, small_in, ring, ids, tab, send, recv, small,
    local_sem, send_sem, tab_sem, ring_sem, ids_sem, row_sem, small_sem, ready,
):
    z, y, x, w = (lax.axis_index(name) for name in (*ROW, "width"))
    far_y, far_x = y // 2, x // 2
    half_y, half_x = y + far_y * (3 - 2 * y), x + far_x * (3 - 2 * x)
    quarter = half_y * 2 + half_x
    block = z * SIDES + quarter

    def owner(slot):
        fy, fx = BLOCKS[slot]
        return NY - 1 - y if fy else y, NX - 1 - x if fx else x

    def gather_peer(slot, core):
        return (z, *owner(slot), core)

    def near_peer(plane, side, core):
        my, mx = BLOCKS[side]
        return (
            plane,
            y + 1 - 2 * lax.rem(y, 2) if my else y,
            x + 1 - 2 * lax.rem(x, 2) if mx else x,
            core,
        )

    def near_line(side):
        my, mx = BLOCKS[side]
        return (1 - half_y if my else half_y) * 2 + (1 - half_x if mx else half_x)

    def z_peer(kz, core):
        return (lax.rem(z + kz, NZ), y, x, core)

    barrier = pltpu.get_barrier_semaphore()
    other = (z, y, x, 1 - w)
    for kz in FAR_Z:
        pl.semaphore_signal(barrier, inc=1, device_id=z_peer(kz, 1), device_id_type=MESH)
    for slot in range(1, OWNERS):
        pl.semaphore_signal(barrier, inc=1, device_id=gather_peer(slot, 0), device_id_type=MESH)
    pl.semaphore_signal(barrier, inc=1, device_id=other, device_id_type=MESH)

    @pl.when(w == 1)
    def _():
        for side in range(1, SIDES):
            peer = near_peer(z, side, 0)
            pl.semaphore_signal(barrier, inc=1, device_id=peer, device_id_type=MESH)


    fetches = [
        pltpu.make_async_copy(src, dst, local_sem.at[i])
        for i, (src, dst) in enumerate(
            (
                (table_hbm, tab.at[0]), (small_hbm, small_in), (ids_hbm, ids_in),
                (sid_hbm, sid), (dense_hbm, dense),
            )
        )
    ]
    for fetch in fetches:
        fetch.start()

    def push(src, dst, kind, sem, peer):
        pltpu.make_async_remote_copy(
            src_ref=src, dst_ref=dst, send_sem=send_sem.at[kind], recv_sem=sem,
            device_id=peer, device_id_type=MESH,
        ).start()

    def wait(ref, sem):
        pltpu.make_async_copy(ref, ref, sem).wait()

    fetches[1].wait()
    two = small_in[...].astype(jnp.float32)
    my_line = small.at[pl.ds((quarter * NZ + z) * OWNERS + far_y * 2 + far_x, 1)]
    my_line[...] = jnp.concatenate([two[0:1], two[1:2], two[0:1], two[1:2]], axis=1)
    fetches[2].wait()
    pair = ids_in[...]
    line = jnp.concatenate([pair[0:1], pair[1:2], pair[0:1], pair[1:2]], axis=1)
    my_ring = ring.at[pl.ds(quarter, 1)]
    my_ring[...] = line
    fetches[0].wait()
    fetches[3].wait()
    fetches[4].wait()
    out_ref[0] = dense[...].astype(jnp.bfloat16)

    @pl.when(w == 0)
    def _():
        pl.semaphore_wait(barrier, 2 * (OWNERS - 1) + SIDES)
        pl.semaphore_signal(ready, inc=1, device_id=other, device_id_type=MESH)

    @pl.when(w == 1)
    def _():
        pl.semaphore_wait(ready, 1)
        for side in FAR_SIDE[:-1]:
            push(my_ring, my_ring, 0, ring_sem.at[0], near_peer(z, side, 1))

    for slot in range(1, OWNERS):
        push(my_line, my_line, 3, small_sem.at[0], gather_peer(slot, w))
    for slot in range(OWNERS - 1, 0, -1):
        push(tab.at[0], tab.at[slot], 1, tab_sem.at[0], gather_peer(slot, w))

    @pl.when(w == 1)
    def _():
        bundle = ids.at[pl.ds(z * SIDES, SIDES)]
        pl.semaphore_wait(barrier, 2 * (NZ - 1) + 1)
        wait(ring.at[pl.ds(0, SIDES - 1)], ring_sem.at[0])
        for kz in FAR_Z:
            for core in (1, 0):
                push(ring, bundle, 0, ids_sem.at[z], z_peer(kz, core))
        push(ring, bundle, 0, ids_sem.at[z], other)
        pl.semaphore_signal(ready, inc=1, device_id=other, device_id_type=MESH)
        pltpu.make_async_copy(ring, bundle, ids_sem.at[z]).start()

    @pl.when(w == 0)
    def _():
        pl.semaphore_wait(ready, 1)

    wait(small.at[pl.ds(0, OWNERS - 1)], small_sem.at[0])
    my_block = small.at[pl.ds((quarter * NZ + z) * OWNERS, OWNERS)]
    my_column = small.at[pl.ds(quarter * NZ * OWNERS, NZ * OWNERS)]
    for kz in FAR_Z:
        push(my_block, my_block, 3, small_sem.at[1], z_peer(kz, w))

    lane = lax.broadcasted_iota(jnp.int32, (1, 128), 1)
    low_half = lane < 64
    low_half16 = lax.broadcasted_iota(jnp.int32, (16, 128), 1) < 64
    low_rows = lax.broadcasted_iota(jnp.int32, (LOW, WIDE), 0)

    for plane in range(NZ):
        wait(ids.at[pl.ds(plane * SIDES, SIDES)], ids_sem.at[plane])
        lines = [ids[pl.ds(plane * SIDES + near_line(side), 1), :] for side in range(SIDES)]
        wanted = jnp.concatenate(
            [jnp.where(low_half, a, b) for a, b in zip(lines[::2], lines[1::2])], axis=1
        )
        high = wanted >> 8
        hot = jnp.where(low_rows == (wanted & (LOW - 1)), 1.0, 0.0).astype(jnp.bfloat16)
        if plane == 0:
            wait(tab.at[pl.ds(1, OWNERS - 1)], tab_sem.at[0])
        lhs = jnp.concatenate(
            [tab[j, :, b * LOW : (b + 1) * LOW] for j in range(OWNERS) for b in range(HIGH)], axis=0
        )
        found = jnp.dot(lhs, hot, preferred_element_type=jnp.float32)
        rows = jnp.zeros((F, WIDE), jnp.float32)
        for j in range(OWNERS):
            yo, xo = owner(j)
            for b in range(HIGH):
                at = (j * HIGH + b) * F
                here = ((z * NY + yo) * NX + xo) * HIGH + b
                rows = jnp.where(high == here, found[at : at + F], rows)
        for half in range(SIDES // 2):
            part = rows[:, half * 128 : (half + 1) * 128]
            upper, lower = part[:16], part[16:]
            turned_upper = pltpu.roll(upper, 64, 1)
            turned_lower = pltpu.roll(lower, 64, 1)
            slot = plane * SIDES + 2 * half
            send[slot] = jnp.where(low_half16, upper, turned_lower).astype(jnp.bfloat16)
            send[slot + 1] = jnp.where(low_half16, turned_upper, lower).astype(jnp.bfloat16)
        for side in FAR_SIDE:
            source, target = send.at[plane * SIDES + side], recv.at[block]
            if side:
                push(source, target, 2, row_sem.at[0], near_peer(plane, side, w))
                continue

            @pl.when(plane != z)
            def _():
                push(source, target, 2, row_sem.at[0], near_peer(plane, side, w))

            @pl.when(plane == z)
            def _():
                pltpu.make_async_copy(source, target, row_sem.at[0]).start()

        if plane < 3:
            continue

        @pl.when(jnp.maximum(z, 3) == plane)
        def _():
            wait(small.at[pl.ds(0, OWNERS * (NZ - 1))], small_sem.at[1])
            for side in range(1, SIDES):
                push(my_column, my_column, 3, small_sem.at[2], near_peer(z, side, w))

    wait(small.at[pl.ds(0, OWNERS * NZ * (SIDES - 1))], small_sem.at[2])
    wanted = sid[...]
    device = wanted >> 1
    high_bits = device >> 1
    folded = device ^ high_bits
    column = ((folded >> 1) & 2) | (folded & 1)
    line = column * (NZ * OWNERS) + (device >> 4) * OWNERS + (((high_bits >> 1) & 2) | (high_bits & 1))
    lines = small[...].astype(jnp.bfloat16)
    small_rows = jnp.zeros((EX, F), jnp.float32)
    for row in range(2):
        spot = jnp.where((wanted & 1) == row, line, -1)
        small_hot = jnp.where(
            lax.broadcasted_iota(jnp.int32, (OWNERS * PEERS, EX), 0) == spot, 1.0, 0.0
        ).astype(jnp.bfloat16)
        small_rows = small_rows + lax.dot_general(
            small_hot, lines[:, row * F : (row + 1) * F], (((0,), (0,)), ((), ())),
            preferred_element_type=jnp.float32,
        )
    out_ref[2] = small_rows.astype(jnp.bfloat16)

    @pl.when(w == 1)
    def _():
        wait(ids.at[pl.ds(0, PEERS)], send_sem.at[0])
        wait(ids.at[pl.ds(0, PEERS - 1)], send_sem.at[0])

    wait(tab.at[pl.ds(1, OWNERS - 1)], send_sem.at[1])
    wait(small.at[pl.ds(0, OWNERS * PEERS - 1)], send_sem.at[3])
    wait(send.at[pl.ds(1, PEERS - 1)], send_sem.at[2])
    wait(recv.at[pl.ds(0, PEERS)], row_sem.at[0])
    total = recv[0].astype(jnp.float32)
    for slot in range(1, PEERS):
        total = total + recv[slot].astype(jnp.float32)
    both = jnp.concatenate(
        [jnp.where(low_half16, total, 0.0), jnp.where(low_half16, 0.0, total)], axis=0
    ).astype(jnp.bfloat16)
    example = lax.broadcasted_iota(jnp.int32, (EX, 128), 0)
    spot = lax.broadcasted_iota(jnp.int32, (EX, 128), 1)
    picks = jnp.where((spot & (EX - 1)) == example, 1.0, 0.0).astype(jnp.bfloat16)
    pooled = lax.dot_general(
        picks, both, (((1,), (1,)), ((), ())), preferred_element_type=jnp.float32
    )
    out_ref[1] = (pooled * 2 ** (-0.5)).astype(jnp.bfloat16)


def shards(row_numbers, item_table, dense_part, small_ids, small_table):
    dma = pltpu.SemaphoreType.DMA
    arrays = row_numbers.T, item_table.T, dense_part, small_ids.reshape(1, EX), small_table
    parts = pl.pallas_call(
        kernel,
        out_shape=jax.ShapeDtypeStruct((3, EX, F), jnp.bfloat16),
        in_specs=[pl.BlockSpec(memory_space=pltpu.HBM)] * 5,
        out_specs=pl.BlockSpec(memory_space=pltpu.VMEM),
        scratch_shapes=[
            pltpu.VMEM((2, EX), jnp.int32),
            pltpu.VMEM((EX, F), jnp.float32),
            pltpu.VMEM((1, EX), jnp.int32),
            pltpu.VMEM((2, F), jnp.bfloat16),
            pltpu.VMEM((SIDES, 128), jnp.int32),
            pltpu.VMEM((PEERS, 128), jnp.int32),
            pltpu.VMEM((OWNERS, F, ROWS), jnp.bfloat16),
            pltpu.VMEM((PEERS, 16, 128), jnp.bfloat16),
            pltpu.VMEM((PEERS, 16, 128), jnp.bfloat16),
            pltpu.VMEM((OWNERS * PEERS, 128), jnp.float32),
            dma((5,)), dma((4,)), dma((1,)), dma((1,)), dma((NZ,)), dma((1,)), dma((3,)),
            pltpu.SemaphoreType.REGULAR,
        ],
        compiler_params=pltpu.CompilerParams(
            collective_id=0, has_side_effects=True, vmem_limit_bytes=16 * 2**20
        ),
    )(*(pltpu.with_memory_space_constraint(array, pltpu.HBM) for array in arrays))
    return parts.transpose(1, 0, 2)


def solution(mesh):
    torus = Mesh(mesh.devices.reshape(NZ, NY, NX, 2), (*ROW, "width"))
    return jax.shard_map(
        shards,
        mesh=torus,
        in_specs=(P(ROW, None), P(ROW, "width"), P(ROW, "width"), P(ROW), P(ROW, "width")),
        out_specs=P(ROW, None, "width"),
        check_vma=False,
    )
```

```python
import jax
import jax.numpy as jnp
from jax import lax
from jax.experimental import pallas as pl
from jax.experimental.pallas import tpu as pltpu
from jax.sharding import Mesh
from jax.sharding import PartitionSpec as P

ROW = ("row_0", "row_1", "row_2")
NZ, NY, NX = 8, 4, 4
MESH = pl.DeviceIdType.MESH
BLOCKS = ((0, 0), (0, 1), (1, 0), (1, 1))
OWNERS = len(BLOCKS)
SIDES = len(BLOCKS)
PEERS = NZ * SIDES
FAR_Z = (4, 3, 5, 2, 6, 1, 7)
FAR_SIDE = (3, 1, 2, 0)
ROWS = 1024
LOW = 256
HIGH = ROWS // LOW
EX = 32
F = 32
WIDE = SIDES * 64


def kernel(
    ids_hbm, table_hbm, dense_hbm, sid_hbm, small_hbm, out_ref,
    ids_in, dense, sid, small_in, ring, ids, tab, send, recv, small,
    local_sem, send_sem, tab_sem, ring_sem, ids_sem, row_sem, small_sem, ready,
):
    z, y, x, w = (lax.axis_index(name) for name in (*ROW, "width"))
    far_y, far_x = y // 2, x // 2
    half_y, half_x = y + far_y * (3 - 2 * y), x + far_x * (3 - 2 * x)
    quarter = half_y * 2 + half_x
    block = z * SIDES + quarter

    def owner(slot):
        fy, fx = BLOCKS[slot]
        return NY - 1 - y if fy else y, NX - 1 - x if fx else x

    def gather_peer(slot, core):
        return (z, *owner(slot), core)

    def near_peer(plane, side, core):
        my, mx = BLOCKS[side]
        return (
            plane,
            y + 1 - 2 * lax.rem(y, 2) if my else y,
            x + 1 - 2 * lax.rem(x, 2) if mx else x,
            core,
        )

    def near_line(side):
        my, mx = BLOCKS[side]
        return (1 - half_y if my else half_y) * 2 + (1 - half_x if mx else half_x)

    def z_peer(kz, core):
        return (lax.rem(z + kz, NZ), y, x, core)

    barrier = pltpu.get_barrier_semaphore()
    other = (z, y, x, 1 - w)
    for kz in FAR_Z:
        pl.semaphore_signal(barrier, inc=1, device_id=z_peer(kz, 1), device_id_type=MESH)
    for slot in range(1, OWNERS):
        pl.semaphore_signal(barrier, inc=1, device_id=gather_peer(slot, 0), device_id_type=MESH)
    pl.semaphore_signal(barrier, inc=1, device_id=other, device_id_type=MESH)

    @pl.when(w == 1)
    def _():
        for side in range(1, SIDES):
            peer = near_peer(z, side, 0)
            pl.semaphore_signal(barrier, inc=1, device_id=peer, device_id_type=MESH)


    fetches = [
        pltpu.make_async_copy(src, dst, local_sem.at[i])
        for i, (src, dst) in enumerate(
            (
                (table_hbm, tab.at[0]), (small_hbm, small_in), (ids_hbm, ids_in),
                (sid_hbm, sid), (dense_hbm, dense),
            )
        )
    ]
    for fetch in fetches:
        fetch.start()

    def push(src, dst, kind, sem, peer):
        pltpu.make_async_remote_copy(
            src_ref=src, dst_ref=dst, send_sem=send_sem.at[kind], recv_sem=sem,
            device_id=peer, device_id_type=MESH,
        ).start()

    def wait(ref, sem):
        pltpu.make_async_copy(ref, ref, sem).wait()

    fetches[1].wait()
    two = small_in[...].astype(jnp.float32)
    my_line = small.at[pl.ds((quarter * NZ + z) * OWNERS + far_y * 2 + far_x, 1)]
    my_line[...] = jnp.concatenate([two[0:1], two[1:2], two[0:1], two[1:2]], axis=1)
    fetches[2].wait()
    pair = ids_in[...]
    line = jnp.concatenate([pair[0:1], pair[1:2], pair[0:1], pair[1:2]], axis=1)
    my_ring = ring.at[pl.ds(quarter, 1)]
    my_ring[...] = line
    fetches[0].wait()
    fetches[3].wait()
    fetches[4].wait()
    out_ref[0] = dense[...].astype(jnp.bfloat16)

    @pl.when(w == 0)
    def _():
        pl.semaphore_wait(barrier, 2 * (OWNERS - 1) + SIDES)
        pl.semaphore_signal(ready, inc=1, device_id=other, device_id_type=MESH)

    @pl.when(w == 1)
    def _():
        pl.semaphore_wait(ready, 1)
        for side in FAR_SIDE[:-1]:
            push(my_ring, my_ring, 0, ring_sem.at[0], near_peer(z, side, 1))

    for slot in range(1, OWNERS):
        push(my_line, my_line, 3, small_sem.at[0], gather_peer(slot, w))
    for slot in range(OWNERS - 1, 0, -1):
        push(tab.at[0], tab.at[slot], 1, tab_sem.at[slot // 3], gather_peer(slot, w))

    @pl.when(w == 1)
    def _():
        bundle = ids.at[pl.ds(z * SIDES, SIDES)]
        pl.semaphore_wait(barrier, 2 * (NZ - 1) + 1)
        wait(ring.at[pl.ds(0, SIDES - 1)], ring_sem.at[0])
        for kz in FAR_Z:
            for core in (1, 0):
                push(ring, bundle, 0, ids_sem.at[z], z_peer(kz, core))
        push(ring, bundle, 0, ids_sem.at[z], other)
        pl.semaphore_signal(ready, inc=1, device_id=other, device_id_type=MESH)
        pltpu.make_async_copy(ring, bundle, ids_sem.at[z]).start()

    @pl.when(w == 0)
    def _():
        pl.semaphore_wait(ready, 1)

    wait(small.at[pl.ds(0, OWNERS - 1)], small_sem.at[0])
    my_block = small.at[pl.ds((quarter * NZ + z) * OWNERS, OWNERS)]
    my_column = small.at[pl.ds(quarter * NZ * OWNERS, NZ * OWNERS)]
    for kz in FAR_Z:
        push(my_block, my_block, 3, small_sem.at[1], z_peer(kz, w))

    lane = lax.broadcasted_iota(jnp.int32, (1, 128), 1)
    low_half = lane < 64
    low_half16 = lax.broadcasted_iota(jnp.int32, (16, 128), 1) < 64
    low_rows = lax.broadcasted_iota(jnp.int32, (LOW, WIDE), 0)

    for plane in range(NZ):
        wait(ids.at[pl.ds(plane * SIDES, SIDES)], ids_sem.at[plane])
        lines = [ids[pl.ds(plane * SIDES + near_line(side), 1), :] for side in range(SIDES)]
        wanted = jnp.concatenate(
            [jnp.where(low_half, a, b) for a, b in zip(lines[::2], lines[1::2])], axis=1
        )
        high = wanted >> 8
        hot = jnp.where(low_rows == (wanted & (LOW - 1)), 1.0, 0.0).astype(jnp.bfloat16)
        rows = jnp.zeros((F, WIDE), jnp.float32)
        for slots in ((0, 1, 2), (3,)) if plane == 0 else ((0, 1), (2, 3)):
            if plane == 0:
                first = max(slots[0], 1)
                wait(tab.at[pl.ds(first, slots[-1] - first + 1)], tab_sem.at[first // 3])
            lhs = jnp.concatenate(
                [tab[j, :, b * LOW : (b + 1) * LOW] for j in slots for b in range(HIGH)], axis=0
            )
            found = jnp.dot(lhs, hot, preferred_element_type=jnp.float32)
            at = 0
            for j in slots:
                yo, xo = owner(j)
                for b in range(HIGH):
                    here = ((z * NY + yo) * NX + xo) * HIGH + b
                    rows = jnp.where(high == here, found[at : at + F], rows)
                    at += F
        for half in range(SIDES // 2):
            part = rows[:, half * 128 : (half + 1) * 128]
            upper, lower = part[:16], part[16:]
            turned_upper = pltpu.roll(upper, 64, 1)
            turned_lower = pltpu.roll(lower, 64, 1)
            slot = plane * SIDES + 2 * half
            send[slot] = jnp.where(low_half16, upper, turned_lower).astype(jnp.bfloat16)
            send[slot + 1] = jnp.where(low_half16, turned_upper, lower).astype(jnp.bfloat16)
        for side in FAR_SIDE:
            source, target = send.at[plane * SIDES + side], recv.at[block]
            if side:
                push(source, target, 2, row_sem.at[0], near_peer(plane, side, w))
                continue

            @pl.when(plane != z)
            def _():
                push(source, target, 2, row_sem.at[0], near_peer(plane, side, w))

            @pl.when(plane == z)
            def _():
                pltpu.make_async_copy(source, target, row_sem.at[0]).start()

        if plane < 3:
            continue

        @pl.when(jnp.maximum(z, 3) == plane)
        def _():
            wait(small.at[pl.ds(0, OWNERS * (NZ - 1))], small_sem.at[1])
            for side in range(1, SIDES):
                push(my_column, my_column, 3, small_sem.at[2], near_peer(z, side, w))

    @pl.when(w == 1)
    def _():
        wait(ids.at[pl.ds(0, PEERS)], send_sem.at[0])
        wait(ids.at[pl.ds(0, PEERS - 1)], send_sem.at[0])

    wait(tab.at[pl.ds(1, OWNERS - 1)], send_sem.at[1])
    wait(small.at[pl.ds(0, OWNERS * PEERS - 1)], send_sem.at[3])
    wait(send.at[pl.ds(1, PEERS - 1)], send_sem.at[2])
    wait(recv.at[pl.ds(0, PEERS)], row_sem.at[0])
    wait(small.at[pl.ds(0, OWNERS * NZ * (SIDES - 1))], small_sem.at[2])
    wanted = sid[...]
    device = wanted >> 1
    high_bits = device >> 1
    folded = device ^ high_bits
    column = ((folded >> 1) & 2) | (folded & 1)
    line = column * (NZ * OWNERS) + (device >> 4) * OWNERS + (((high_bits >> 1) & 2) | (high_bits & 1))
    lines = small[...].astype(jnp.bfloat16)
    small_rows = jnp.zeros((EX, F), jnp.float32)
    for row in range(2):
        spot = jnp.where((wanted & 1) == row, line, -1)
        small_hot = jnp.where(
            lax.broadcasted_iota(jnp.int32, (OWNERS * PEERS, EX), 0) == spot, 1.0, 0.0
        ).astype(jnp.bfloat16)
        small_rows = small_rows + lax.dot_general(
            small_hot, lines[:, row * F : (row + 1) * F], (((0,), (0,)), ((), ())),
            preferred_element_type=jnp.float32,
        )
    out_ref[2] = small_rows.astype(jnp.bfloat16)

    total = recv[0].astype(jnp.float32)
    for slot in range(1, PEERS):
        total = total + recv[slot].astype(jnp.float32)
    both = jnp.concatenate(
        [jnp.where(low_half16, total, 0.0), jnp.where(low_half16, 0.0, total)], axis=0
    ).astype(jnp.bfloat16)
    example = lax.broadcasted_iota(jnp.int32, (EX, 128), 0)
    spot = lax.broadcasted_iota(jnp.int32, (EX, 128), 1)
    picks = jnp.where((spot & (EX - 1)) == example, 1.0, 0.0).astype(jnp.bfloat16)
    pooled = lax.dot_general(
        picks, both, (((1,), (1,)), ((), ())), preferred_element_type=jnp.float32
    )
    out_ref[1] = (pooled * 2 ** (-0.5)).astype(jnp.bfloat16)


def shards(row_numbers, item_table, dense_part, small_ids, small_table):
    dma = pltpu.SemaphoreType.DMA
    arrays = row_numbers.T, item_table.T, dense_part, small_ids.reshape(1, EX), small_table
    parts = pl.pallas_call(
        kernel,
        out_shape=jax.ShapeDtypeStruct((3, EX, F), jnp.bfloat16),
        in_specs=[pl.BlockSpec(memory_space=pltpu.HBM)] * 5,
        out_specs=pl.BlockSpec(memory_space=pltpu.VMEM),
        scratch_shapes=[
            pltpu.VMEM((2, EX), jnp.int32),
            pltpu.VMEM((EX, F), jnp.float32),
            pltpu.VMEM((1, EX), jnp.int32),
            pltpu.VMEM((2, F), jnp.bfloat16),
            pltpu.VMEM((SIDES, 128), jnp.int32),
            pltpu.VMEM((PEERS, 128), jnp.int32),
            pltpu.VMEM((OWNERS, F, ROWS), jnp.bfloat16),
            pltpu.VMEM((PEERS, 16, 128), jnp.bfloat16),
            pltpu.VMEM((PEERS, 16, 128), jnp.bfloat16),
            pltpu.VMEM((OWNERS * PEERS, 128), jnp.float32),
            dma((5,)), dma((4,)), dma((2,)), dma((1,)), dma((NZ,)), dma((1,)), dma((3,)),
            pltpu.SemaphoreType.REGULAR,
        ],
        compiler_params=pltpu.CompilerParams(
            collective_id=0, has_side_effects=True, vmem_limit_bytes=16 * 2**20
        ),
    )(*(pltpu.with_memory_space_constraint(array, pltpu.HBM) for array in arrays))
    return parts.transpose(1, 0, 2)


def solution(mesh):
    torus = Mesh(mesh.devices.reshape(NZ, NY, NX, 2), (*ROW, "width"))
    return jax.shard_map(
        shards,
        mesh=torus,
        in_specs=(P(ROW, None), P(ROW, "width"), P(ROW, "width"), P(ROW), P(ROW, "width")),
        out_specs=P(ROW, None, "width"),
        check_vma=False,
    )
```

```python
import jax
import jax.numpy as jnp
from jax import lax
from jax.experimental import pallas as pl
from jax.experimental.pallas import tpu as pltpu
from jax.sharding import Mesh
from jax.sharding import PartitionSpec as P

ROW = ("row_0", "row_1", "row_2")
NZ, NY, NX = 8, 4, 4
MESH = pl.DeviceIdType.MESH
BLOCKS = ((0, 0), (0, 1), (1, 0), (1, 1))
OWNERS = len(BLOCKS)
SIDES = len(BLOCKS)
PEERS = NZ * SIDES
FAR_Z = (4, 3, 5, 2, 6, 1, 7)
FAR_SIDE = (3, 1, 2, 0)
ROWS = 1024
LOW = 256
HIGH = ROWS // LOW
EX = 32
F = 32
WIDE = SIDES * 64


def kernel(
    ids_hbm, table_hbm, dense_hbm, sid_hbm, small_hbm, out_ref,
    ids_in, dense, sid, small_in, ring, ids, tab, send, recv, small,
    local_sem, send_sem, tab_sem, ring_sem, ids_sem, row_sem, small_sem, ready,
):
    z, y, x, w = (lax.axis_index(name) for name in (*ROW, "width"))
    far_y, far_x = y // 2, x // 2
    half_y, half_x = y + far_y * (3 - 2 * y), x + far_x * (3 - 2 * x)
    quarter = half_y * 2 + half_x
    block = z * SIDES + quarter

    def owner(slot):
        fy, fx = BLOCKS[slot]
        return NY - 1 - y if fy else y, NX - 1 - x if fx else x

    def gather_peer(slot, core):
        return (z, *owner(slot), core)

    def near_peer(plane, side, core):
        my, mx = BLOCKS[side]
        return (
            plane,
            y + 1 - 2 * lax.rem(y, 2) if my else y,
            x + 1 - 2 * lax.rem(x, 2) if mx else x,
            core,
        )

    def near_line(side):
        my, mx = BLOCKS[side]
        return (1 - half_y if my else half_y) * 2 + (1 - half_x if mx else half_x)

    def z_peer(kz, core):
        return (lax.rem(z + kz, NZ), y, x, core)

    barrier = pltpu.get_barrier_semaphore()
    other = (z, y, x, 1 - w)
    for kz in FAR_Z:
        pl.semaphore_signal(barrier, inc=1, device_id=z_peer(kz, 1), device_id_type=MESH)
    for slot in range(1, OWNERS):
        pl.semaphore_signal(barrier, inc=1, device_id=gather_peer(slot, 0), device_id_type=MESH)
    pl.semaphore_signal(barrier, inc=1, device_id=other, device_id_type=MESH)

    for side in range(1, SIDES):
        pl.semaphore_signal(barrier, inc=1, device_id=near_peer(z, side, 0), device_id_type=MESH)


    fetches = [
        pltpu.make_async_copy(src, dst, local_sem.at[i])
        for i, (src, dst) in enumerate(
            (
                (table_hbm, tab.at[0]), (small_hbm, small_in), (ids_hbm, ids_in),
                (sid_hbm, sid), (dense_hbm, dense),
            )
        )
    ]
    for fetch in fetches:
        fetch.start()

    def push(src, dst, kind, sem, peer):
        pltpu.make_async_remote_copy(
            src_ref=src, dst_ref=dst, send_sem=send_sem.at[kind], recv_sem=sem,
            device_id=peer, device_id_type=MESH,
        ).start()

    def wait(ref, sem):
        pltpu.make_async_copy(ref, ref, sem).wait()

    fetches[1].wait()
    two = small_in[...].astype(jnp.float32)
    far = far_y * 2 + far_x
    my_line = small.at[pl.ds((far * NZ + z) * SIDES + quarter, 1)]
    my_line[...] = jnp.concatenate([two[0:1], two[1:2], two[0:1], two[1:2]], axis=1)
    fetches[2].wait()
    pair = ids_in[...]
    line = jnp.concatenate([pair[0:1], pair[1:2], pair[0:1], pair[1:2]], axis=1)
    my_ring = ring.at[pl.ds(quarter, 1)]
    my_ring[...] = line
    fetches[0].wait()
    fetches[3].wait()
    fetches[4].wait()
    out_ref[0] = dense[...].astype(jnp.bfloat16)

    @pl.when(w == 0)
    def _():
        pl.semaphore_wait(barrier, 2 * (OWNERS + SIDES - 2) + 1)
        pl.semaphore_signal(ready, inc=1, device_id=other, device_id_type=MESH)

    @pl.when(w == 1)
    def _():
        pl.semaphore_wait(ready, 1)
        for side in FAR_SIDE[:-1]:
            push(my_ring, my_ring, 0, ring_sem.at[0], near_peer(z, side, 1))

    for side in range(1, SIDES):
        push(my_line, my_line, 3, small_sem.at[0], near_peer(z, side, w))
    for slot in range(OWNERS - 1, 0, -1):
        push(tab.at[0], tab.at[slot], 1, tab_sem.at[slot // 3], gather_peer(slot, w))

    @pl.when(w == 1)
    def _():
        bundle = ids.at[pl.ds(z * SIDES, SIDES)]
        pl.semaphore_wait(barrier, 2 * (NZ - 1) + 1)
        wait(ring.at[pl.ds(0, SIDES - 1)], ring_sem.at[0])
        for kz in FAR_Z:
            for core in (1, 0):
                push(ring, bundle, 0, ids_sem.at[z], z_peer(kz, core))
        push(ring, bundle, 0, ids_sem.at[z], other)
        pl.semaphore_signal(ready, inc=1, device_id=other, device_id_type=MESH)
        pltpu.make_async_copy(ring, bundle, ids_sem.at[z]).start()

    @pl.when(w == 0)
    def _():
        pl.semaphore_wait(ready, 1)

    wait(small.at[pl.ds(0, OWNERS - 1)], small_sem.at[0])
    my_block = small.at[pl.ds((far * NZ + z) * SIDES, SIDES)]
    my_column = small.at[pl.ds(far * NZ * SIDES, NZ * SIDES)]
    for kz in FAR_Z:
        push(my_block, my_block, 3, small_sem.at[1], z_peer(kz, w))

    lane = lax.broadcasted_iota(jnp.int32, (1, 128), 1)
    low_half = lane < 64
    low_half16 = lax.broadcasted_iota(jnp.int32, (16, 128), 1) < 64
    low_rows = lax.broadcasted_iota(jnp.int32, (LOW, WIDE), 0)

    for plane in range(NZ):
        wait(ids.at[pl.ds(plane * SIDES, SIDES)], ids_sem.at[plane])
        lines = [ids[pl.ds(plane * SIDES + near_line(side), 1), :] for side in range(SIDES)]
        wanted = jnp.concatenate(
            [jnp.where(low_half, a, b) for a, b in zip(lines[::2], lines[1::2])], axis=1
        )
        high = wanted >> 8
        hot = jnp.where(low_rows == (wanted & (LOW - 1)), 1.0, 0.0).astype(jnp.bfloat16)
        rows = jnp.zeros((F, WIDE), jnp.float32)
        for slots in ((0, 1, 2), (3,)) if plane == 0 else ((0, 1), (2, 3)):
            if plane == 0:
                first = max(slots[0], 1)
                wait(tab.at[pl.ds(first, slots[-1] - first + 1)], tab_sem.at[first // 3])
            lhs = jnp.concatenate(
                [tab[j, :, b * LOW : (b + 1) * LOW] for j in slots for b in range(HIGH)], axis=0
            )
            found = jnp.dot(lhs, hot, preferred_element_type=jnp.float32)
            at = 0
            for j in slots:
                yo, xo = owner(j)
                for b in range(HIGH):
                    here = ((z * NY + yo) * NX + xo) * HIGH + b
                    rows = jnp.where(high == here, found[at : at + F], rows)
                    at += F
        for half in range(SIDES // 2):
            part = rows[:, half * 128 : (half + 1) * 128]
            upper, lower = part[:16], part[16:]
            turned_upper = pltpu.roll(upper, 64, 1)
            turned_lower = pltpu.roll(lower, 64, 1)
            slot = plane * SIDES + 2 * half
            send[slot] = jnp.where(low_half16, upper, turned_lower).astype(jnp.bfloat16)
            send[slot + 1] = jnp.where(low_half16, turned_upper, lower).astype(jnp.bfloat16)
        for side in FAR_SIDE:
            source, target = send.at[plane * SIDES + side], recv.at[block]
            if side:
                push(source, target, 2, row_sem.at[0], near_peer(plane, side, w))
                continue

            @pl.when(plane != z)
            def _():
                push(source, target, 2, row_sem.at[0], near_peer(plane, side, w))

            @pl.when(plane == z)
            def _():
                pltpu.make_async_copy(source, target, row_sem.at[0]).start()

        if plane == 3:
            wait(small.at[pl.ds(0, OWNERS * (NZ - 1))], small_sem.at[1])
            for slot in range(1, OWNERS):
                push(my_column, my_column, 3, small_sem.at[2], gather_peer(slot, w))

    @pl.when(w == 1)
    def _():
        wait(ids.at[pl.ds(0, PEERS)], send_sem.at[0])
        wait(ids.at[pl.ds(0, PEERS - 1)], send_sem.at[0])

    wait(tab.at[pl.ds(1, OWNERS - 1)], send_sem.at[1])
    wait(small.at[pl.ds(0, OWNERS * PEERS - 1)], send_sem.at[3])
    wait(send.at[pl.ds(1, PEERS - 1)], send_sem.at[2])
    wait(recv.at[pl.ds(0, PEERS)], row_sem.at[0])
    wait(small.at[pl.ds(0, OWNERS * NZ * (SIDES - 1))], small_sem.at[2])
    wanted = sid[...]
    device = wanted >> 1
    high_bits = device >> 1
    folded = device ^ high_bits
    column = ((folded >> 1) & 2) | (folded & 1)
    line = ((((high_bits >> 1) & 2) | (high_bits & 1)) * NZ + (device >> 4)) * SIDES + column
    lines = small[...].astype(jnp.bfloat16)
    small_rows = jnp.zeros((EX, F), jnp.float32)
    for row in range(2):
        spot = jnp.where((wanted & 1) == row, line, -1)
        small_hot = jnp.where(
            lax.broadcasted_iota(jnp.int32, (OWNERS * PEERS, EX), 0) == spot, 1.0, 0.0
        ).astype(jnp.bfloat16)
        small_rows = small_rows + lax.dot_general(
            small_hot, lines[:, row * F : (row + 1) * F], (((0,), (0,)), ((), ())),
            preferred_element_type=jnp.float32,
        )
    out_ref[2] = small_rows.astype(jnp.bfloat16)

    total = recv[0].astype(jnp.float32)
    for slot in range(1, PEERS):
        total = total + recv[slot].astype(jnp.float32)
    both = jnp.concatenate(
        [jnp.where(low_half16, total, 0.0), jnp.where(low_half16, 0.0, total)], axis=0
    ).astype(jnp.bfloat16)
    example = lax.broadcasted_iota(jnp.int32, (EX, 128), 0)
    spot = lax.broadcasted_iota(jnp.int32, (EX, 128), 1)
    picks = jnp.where((spot & (EX - 1)) == example, 1.0, 0.0).astype(jnp.bfloat16)
    pooled = lax.dot_general(
        picks, both, (((1,), (1,)), ((), ())), preferred_element_type=jnp.float32
    )
    out_ref[1] = (pooled * 2 ** (-0.5)).astype(jnp.bfloat16)


def shards(row_numbers, item_table, dense_part, small_ids, small_table):
    dma = pltpu.SemaphoreType.DMA
    arrays = row_numbers.T, item_table.T, dense_part, small_ids.reshape(1, EX), small_table
    parts = pl.pallas_call(
        kernel,
        out_shape=jax.ShapeDtypeStruct((3, EX, F), jnp.bfloat16),
        in_specs=[pl.BlockSpec(memory_space=pltpu.HBM)] * 5,
        out_specs=pl.BlockSpec(memory_space=pltpu.VMEM),
        scratch_shapes=[
            pltpu.VMEM((2, EX), jnp.int32),
            pltpu.VMEM((EX, F), jnp.float32),
            pltpu.VMEM((1, EX), jnp.int32),
            pltpu.VMEM((2, F), jnp.bfloat16),
            pltpu.VMEM((SIDES, 128), jnp.int32),
            pltpu.VMEM((PEERS, 128), jnp.int32),
            pltpu.VMEM((OWNERS, F, ROWS), jnp.bfloat16),
            pltpu.VMEM((PEERS, 16, 128), jnp.bfloat16),
            pltpu.VMEM((PEERS, 16, 128), jnp.bfloat16),
            pltpu.VMEM((OWNERS * PEERS, 128), jnp.float32),
            dma((5,)), dma((4,)), dma((2,)), dma((1,)), dma((NZ,)), dma((1,)), dma((3,)),
            pltpu.SemaphoreType.REGULAR,
        ],
        compiler_params=pltpu.CompilerParams(
            collective_id=0, has_side_effects=True, vmem_limit_bytes=16 * 2**20
        ),
    )(*(pltpu.with_memory_space_constraint(array, pltpu.HBM) for array in arrays))
    return parts.transpose(1, 0, 2)


def solution(mesh):
    torus = Mesh(mesh.devices.reshape(NZ, NY, NX, 2), (*ROW, "width"))
    return jax.shard_map(
        shards,
        mesh=torus,
        in_specs=(P(ROW, None), P(ROW, "width"), P(ROW, "width"), P(ROW), P(ROW, "width")),
        out_specs=P(ROW, None, "width"),
        check_vma=False,
    )
```

```python
import jax
import jax.numpy as jnp
from jax import lax
from jax.experimental import pallas as pl
from jax.experimental.pallas import tpu as pltpu
from jax.sharding import Mesh
from jax.sharding import PartitionSpec as P

ROW = ("row_0", "row_1", "row_2")
NZ, NY, NX = 8, 4, 4
MESH = pl.DeviceIdType.MESH
BLOCKS = ((0, 0), (0, 1), (1, 0), (1, 1))
OWNERS = len(BLOCKS)
SIDES = len(BLOCKS)
PEERS = NZ * SIDES
FAR_Z = (4, 3, 5, 2, 6, 1, 7)
FAR_SIDE = (3, 1, 2, 0)
ROWS = 1024
LOW = 256
HIGH = ROWS // LOW
EX = 32
F = 32
WIDE = SIDES * 64


def kernel(
    ids_hbm, table_hbm, dense_hbm, sid_hbm, small_hbm, out_ref,
    ids_in, dense, sid, small_in, ring, ids, tab, send, recv, small,
    local_sem, send_sem, tab_sem, ring_sem, ids_sem, row_sem, small_sem, ready,
):
    z, y, x, w = (lax.axis_index(name) for name in (*ROW, "width"))
    far_y, far_x = y // 2, x // 2
    half_y, half_x = y + far_y * (3 - 2 * y), x + far_x * (3 - 2 * x)
    quarter = half_y * 2 + half_x
    block = z * SIDES + quarter

    def owner(slot):
        fy, fx = BLOCKS[slot]
        return NY - 1 - y if fy else y, NX - 1 - x if fx else x

    part = z - z // 4 * (z - 4)

    def gather_peer(slot, core):
        return (z, *owner(slot), core)

    def near_peer(plane, side, core):
        my, mx = BLOCKS[side]
        return (
            plane,
            y + 1 - 2 * lax.rem(y, 2) if my else y,
            x + 1 - 2 * lax.rem(x, 2) if mx else x,
            core,
        )

    def near_line(side):
        my, mx = BLOCKS[side]
        return (1 - half_y if my else half_y) * 2 + (1 - half_x if mx else half_x)

    def z_peer(kz, core):
        return (lax.rem(z + kz, NZ), y, x, core)

    barrier = pltpu.get_barrier_semaphore()
    other = (z, y, x, 1 - w)
    for kz in FAR_Z:
        pl.semaphore_signal(barrier, inc=1, device_id=z_peer(kz, 1), device_id_type=MESH)
    for slot in range(1, OWNERS):
        pl.semaphore_signal(barrier, inc=1, device_id=gather_peer(slot, 0), device_id_type=MESH)
    pl.semaphore_signal(barrier, inc=1, device_id=other, device_id_type=MESH)

    for side in range(1, SIDES):
        pl.semaphore_signal(barrier, inc=1, device_id=near_peer(z, side, 0), device_id_type=MESH)


    fetches = [
        pltpu.make_async_copy(src, dst, local_sem.at[i])
        for i, (src, dst) in enumerate(
            (
                (table_hbm, tab.at[0]), (small_hbm, small_in), (ids_hbm, ids_in),
                (sid_hbm, sid), (dense_hbm, dense),
            )
        )
    ]
    for fetch in fetches:
        fetch.start()

    def push(src, dst, kind, sem, peer):
        pltpu.make_async_remote_copy(
            src_ref=src, dst_ref=dst, send_sem=send_sem.at[kind], recv_sem=sem,
            device_id=peer, device_id_type=MESH,
        ).start()

    def wait(ref, sem):
        pltpu.make_async_copy(ref, ref, sem).wait()

    fetches[1].wait()
    two = small_in[...].astype(jnp.float32)
    far = far_y * 2 + far_x
    my_line = small.at[pl.ds((far * NZ + z) * SIDES + quarter, 1)]
    my_line[...] = jnp.concatenate([two[0:1], two[1:2], two[0:1], two[1:2]], axis=1)
    fetches[2].wait()
    pair = ids_in[...]
    line = jnp.concatenate([pair[0:1], pair[1:2], pair[0:1], pair[1:2]], axis=1)
    my_ring = ring.at[pl.ds(quarter, 1)]
    my_ring[...] = line
    fetches[0].wait()
    fetches[3].wait()
    fetches[4].wait()
    out_ref[0] = dense[...].astype(jnp.bfloat16)

    @pl.when(w == 0)
    def _():
        pl.semaphore_wait(barrier, 2 * (OWNERS + SIDES - 2) + 1)
        pl.semaphore_signal(ready, inc=1, device_id=other, device_id_type=MESH)

    @pl.when(w == 1)
    def _():
        pl.semaphore_wait(ready, 1)
        for side in FAR_SIDE[:-1]:
            push(my_ring, my_ring, 0, ring_sem.at[0], near_peer(z, side, 1))

    for side in range(1, SIDES):
        push(my_line, my_line, 3, small_sem.at[0], near_peer(z, side, w))
    for slot in range(OWNERS - 1, 0, -1):
        push(tab.at[0], tab.at[slot], 1, tab_sem.at[slot // 3], gather_peer(slot, w))

    @pl.when(w == 1)
    def _():
        bundle = ids.at[pl.ds(z * SIDES, SIDES)]
        pl.semaphore_wait(barrier, 2 * (NZ - 1) + 1)
        wait(ring.at[pl.ds(0, SIDES - 1)], ring_sem.at[0])
        for kz in FAR_Z:
            for core in (1, 0):
                push(ring, bundle, 0, ids_sem.at[part], z_peer(kz, core))
        push(ring, bundle, 0, ids_sem.at[part], other)
        pl.semaphore_signal(ready, inc=1, device_id=other, device_id_type=MESH)
        pltpu.make_async_copy(ring, bundle, ids_sem.at[part]).start()

    @pl.when(w == 0)
    def _():
        pl.semaphore_wait(ready, 1)

    wait(small.at[pl.ds(0, OWNERS - 1)], small_sem.at[0])
    my_block = small.at[pl.ds((far * NZ + z) * SIDES, SIDES)]
    my_column = small.at[pl.ds(far * NZ * SIDES, NZ * SIDES)]
    for kz in FAR_Z:
        push(my_block, my_block, 3, small_sem.at[1], z_peer(kz, w))

    lane = lax.broadcasted_iota(jnp.int32, (1, 128), 1)
    low_half = lane < 64
    low_half16 = lax.broadcasted_iota(jnp.int32, (16, 128), 1) < 64
    low_rows = lax.broadcasted_iota(jnp.int32, (LOW, WIDE), 0)

    for plane in range(NZ):
        if plane <= 4:
            planes = 1 if plane < 4 else NZ - 4
            wait(ids.at[pl.ds(plane * SIDES, planes * SIDES)], ids_sem.at[plane])
        lines = [ids[pl.ds(plane * SIDES + near_line(side), 1), :] for side in range(SIDES)]
        wanted = jnp.concatenate(
            [jnp.where(low_half, a, b) for a, b in zip(lines[::2], lines[1::2])], axis=1
        )
        high = wanted >> 8
        hot = jnp.where(low_rows == (wanted & (LOW - 1)), 1.0, 0.0).astype(jnp.bfloat16)
        rows = jnp.zeros((F, WIDE), jnp.float32)
        for slots in ((0, 1, 2), (3,)) if plane == 0 else ((0, 1), (2, 3)):
            if plane == 0:
                first = max(slots[0], 1)
                wait(tab.at[pl.ds(first, slots[-1] - first + 1)], tab_sem.at[first // 3])
            lhs = jnp.concatenate(
                [tab[j, :, b * LOW : (b + 1) * LOW] for j in slots for b in range(HIGH)], axis=0
            )
            found = jnp.dot(lhs, hot, preferred_element_type=jnp.float32)
            at = 0
            for j in slots:
                yo, xo = owner(j)
                for b in range(HIGH):
                    here = ((z * NY + yo) * NX + xo) * HIGH + b
                    rows = jnp.where(high == here, found[at : at + F], rows)
                    at += F
        for half in range(SIDES // 2):
            part = rows[:, half * 128 : (half + 1) * 128]
            upper, lower = part[:16], part[16:]
            turned_upper = pltpu.roll(upper, 64, 1)
            turned_lower = pltpu.roll(lower, 64, 1)
            slot = plane * SIDES + 2 * half
            send[slot] = jnp.where(low_half16, upper, turned_lower).astype(jnp.bfloat16)
            send[slot + 1] = jnp.where(low_half16, turned_upper, lower).astype(jnp.bfloat16)
        for side in FAR_SIDE:
            source, target = send.at[plane * SIDES + side], recv.at[block]
            if side:
                push(source, target, 2, row_sem.at[0], near_peer(plane, side, w))
                continue

            @pl.when(plane != z)
            def _():
                push(source, target, 2, row_sem.at[0], near_peer(plane, side, w))

            @pl.when(plane == z)
            def _():
                pltpu.make_async_copy(source, target, row_sem.at[0]).start()

        if plane == 3:
            wait(small.at[pl.ds(0, OWNERS * (NZ - 1))], small_sem.at[1])
            for slot in range(1, OWNERS):
                push(my_column, my_column, 3, small_sem.at[2], gather_peer(slot, w))

    @pl.when(w == 1)
    def _():
        wait(ids.at[pl.ds(0, PEERS)], send_sem.at[0])
        wait(ids.at[pl.ds(0, PEERS - 1)], send_sem.at[0])

    wait(tab.at[pl.ds(1, OWNERS - 1)], send_sem.at[1])
    wait(small.at[pl.ds(0, OWNERS * PEERS - 1)], send_sem.at[3])
    wait(send.at[pl.ds(1, PEERS - 1)], send_sem.at[2])
    wait(recv.at[pl.ds(0, PEERS)], row_sem.at[0])
    wait(small.at[pl.ds(0, OWNERS * NZ * (SIDES - 1))], small_sem.at[2])
    wanted = sid[...]
    device = wanted >> 1
    high_bits = device >> 1
    folded = device ^ high_bits
    column = ((folded >> 1) & 2) | (folded & 1)
    line = ((((high_bits >> 1) & 2) | (high_bits & 1)) * NZ + (device >> 4)) * SIDES + column
    lines = small[...].astype(jnp.bfloat16)
    small_rows = jnp.zeros((EX, F), jnp.float32)
    for row in range(2):
        spot = jnp.where((wanted & 1) == row, line, -1)
        small_hot = jnp.where(
            lax.broadcasted_iota(jnp.int32, (OWNERS * PEERS, EX), 0) == spot, 1.0, 0.0
        ).astype(jnp.bfloat16)
        small_rows = small_rows + lax.dot_general(
            small_hot, lines[:, row * F : (row + 1) * F], (((0,), (0,)), ((), ())),
            preferred_element_type=jnp.float32,
        )
    out_ref[2] = small_rows.astype(jnp.bfloat16)

    total = recv[0].astype(jnp.float32)
    for slot in range(1, PEERS):
        total = total + recv[slot].astype(jnp.float32)
    both = jnp.concatenate(
        [jnp.where(low_half16, total, 0.0), jnp.where(low_half16, 0.0, total)], axis=0
    ).astype(jnp.bfloat16)
    example = lax.broadcasted_iota(jnp.int32, (EX, 128), 0)
    spot = lax.broadcasted_iota(jnp.int32, (EX, 128), 1)
    picks = jnp.where((spot & (EX - 1)) == example, 1.0, 0.0).astype(jnp.bfloat16)
    pooled = lax.dot_general(
        picks, both, (((1,), (1,)), ((), ())), preferred_element_type=jnp.float32
    )
    out_ref[1] = (pooled * 2 ** (-0.5)).astype(jnp.bfloat16)


def shards(row_numbers, item_table, dense_part, small_ids, small_table):
    dma = pltpu.SemaphoreType.DMA
    arrays = row_numbers.T, item_table.T, dense_part, small_ids.reshape(1, EX), small_table
    parts = pl.pallas_call(
        kernel,
        out_shape=jax.ShapeDtypeStruct((3, EX, F), jnp.bfloat16),
        in_specs=[pl.BlockSpec(memory_space=pltpu.HBM)] * 5,
        out_specs=pl.BlockSpec(memory_space=pltpu.VMEM),
        scratch_shapes=[
            pltpu.VMEM((2, EX), jnp.int32),
            pltpu.VMEM((EX, F), jnp.float32),
            pltpu.VMEM((1, EX), jnp.int32),
            pltpu.VMEM((2, F), jnp.bfloat16),
            pltpu.VMEM((SIDES, 128), jnp.int32),
            pltpu.VMEM((PEERS, 128), jnp.int32),
            pltpu.VMEM((OWNERS, F, ROWS), jnp.bfloat16),
            pltpu.VMEM((PEERS, 16, 128), jnp.bfloat16),
            pltpu.VMEM((PEERS, 16, 128), jnp.bfloat16),
            pltpu.VMEM((OWNERS * PEERS, 128), jnp.float32),
            dma((5,)), dma((4,)), dma((2,)), dma((1,)), dma((5,)), dma((1,)), dma((3,)),
            pltpu.SemaphoreType.REGULAR,
        ],
        compiler_params=pltpu.CompilerParams(
            collective_id=0, has_side_effects=True, vmem_limit_bytes=16 * 2**20
        ),
    )(*(pltpu.with_memory_space_constraint(array, pltpu.HBM) for array in arrays))
    return parts.transpose(1, 0, 2)


def solution(mesh):
    torus = Mesh(mesh.devices.reshape(NZ, NY, NX, 2), (*ROW, "width"))
    return jax.shard_map(
        shards,
        mesh=torus,
        in_specs=(P(ROW, None), P(ROW, "width"), P(ROW, "width"), P(ROW), P(ROW, "width")),
        out_specs=P(ROW, None, "width"),
        check_vma=False,
    )
```

```python
import jax
import jax.numpy as jnp
from jax import lax
from jax.experimental import pallas as pl
from jax.experimental.pallas import tpu as pltpu
from jax.sharding import Mesh
from jax.sharding import PartitionSpec as P

ROW = ("row_0", "row_1", "row_2")
NZ, NY, NX = 8, 4, 4
MESH = pl.DeviceIdType.MESH
BLOCKS = ((0, 0), (0, 1), (1, 0), (1, 1))
OWNERS = len(BLOCKS)
SIDES = len(BLOCKS)
PEERS = NZ * SIDES
FAR_Z = (4, 3, 5, 2, 6, 1, 7)
FAR_SIDE = (3, 1, 2, 0)
ROWS = 1024
LOW = 256
HIGH = ROWS // LOW
EX = 32
F = 32
WIDE = SIDES * 64


def kernel(
    ids_hbm, table_hbm, dense_hbm, sid_hbm, small_hbm, out_ref,
    ids_in, dense, sid, small_in, ring, ids, tab, send, recv, small,
    local_sem, send_sem, tab_sem, ring_sem, ids_sem, row_sem, small_sem, ready,
):
    z, y, x, w = (lax.axis_index(name) for name in (*ROW, "width"))
    far_y, far_x = y // 2, x // 2
    half_y, half_x = y + far_y * (3 - 2 * y), x + far_x * (3 - 2 * x)
    quarter = half_y * 2 + half_x
    block = z * SIDES + quarter

    def owner(slot):
        fy, fx = BLOCKS[slot]
        return NY - 1 - y if fy else y, NX - 1 - x if fx else x

    def gather_peer(slot, core):
        return (z, *owner(slot), core)

    def near_peer(plane, side, core):
        my, mx = BLOCKS[side]
        return (
            plane,
            y + 1 - 2 * lax.rem(y, 2) if my else y,
            x + 1 - 2 * lax.rem(x, 2) if mx else x,
            core,
        )

    def near_line(side):
        my, mx = BLOCKS[side]
        return (1 - half_y if my else half_y) * 2 + (1 - half_x if mx else half_x)

    def z_peer(kz, core):
        return (lax.rem(z + kz, NZ), y, x, core)

    barrier = pltpu.get_barrier_semaphore()
    other = (z, y, x, 1 - w)
    for kz in FAR_Z:
        pl.semaphore_signal(barrier, inc=1, device_id=z_peer(kz, 1), device_id_type=MESH)
    for slot in range(1, OWNERS):
        pl.semaphore_signal(barrier, inc=1, device_id=gather_peer(slot, 0), device_id_type=MESH)
    pl.semaphore_signal(barrier, inc=1, device_id=other, device_id_type=MESH)

    for side in range(1, SIDES):
        pl.semaphore_signal(barrier, inc=1, device_id=near_peer(z, side, 0), device_id_type=MESH)


    fetches = [
        pltpu.make_async_copy(src, dst, local_sem.at[i])
        for i, (src, dst) in enumerate(
            (
                (table_hbm, tab.at[0]), (small_hbm, small_in), (ids_hbm, ids_in),
                (sid_hbm, sid), (dense_hbm, dense),
            )
        )
    ]
    for fetch in fetches:
        fetch.start()

    def push(src, dst, kind, sem, peer):
        pltpu.make_async_remote_copy(
            src_ref=src, dst_ref=dst, send_sem=send_sem.at[kind], recv_sem=sem,
            device_id=peer, device_id_type=MESH,
        ).start()

    def wait(ref, sem):
        pltpu.make_async_copy(ref, ref, sem).wait()

    fetches[1].wait()
    two = small_in[...].astype(jnp.float32)
    far = far_y * 2 + far_x
    my_line = small.at[pl.ds((far * NZ + z) * SIDES + quarter, 1)]
    my_line[...] = jnp.concatenate([two[0:1], two[1:2], two[0:1], two[1:2]], axis=1)
    fetches[2].wait()
    pair = ids_in[...]
    line = jnp.concatenate([pair[0:1], pair[1:2], pair[0:1], pair[1:2]], axis=1)
    my_ring = ring.at[pl.ds(quarter, 1)]
    my_ring[...] = line
    fetches[0].wait()
    fetches[3].wait()
    fetches[4].wait()
    out_ref[0] = dense[...].astype(jnp.bfloat16)

    @pl.when(w == 0)
    def _():
        pl.semaphore_wait(barrier, 2 * (OWNERS + SIDES - 2) + 1)
        pl.semaphore_signal(ready, inc=1, device_id=other, device_id_type=MESH)

    @pl.when(w == 1)
    def _():
        pl.semaphore_wait(ready, 1)
        for side in FAR_SIDE[:-1]:
            push(my_ring, my_ring, 0, ring_sem.at[0], near_peer(z, side, 1))

    for side in range(1, SIDES):
        push(my_line, my_line, 3, small_sem.at[0], near_peer(z, side, w))
    for slot in range(OWNERS - 1, 0, -1):
        push(tab.at[0], tab.at[slot], 1, tab_sem.at[slot // 3], gather_peer(slot, w))

    @pl.when(w == 1)
    def _():
        bundle = ids.at[pl.ds(z * SIDES, SIDES)]
        pl.semaphore_wait(barrier, 2 * (NZ - 1) + 1)
        wait(ring.at[pl.ds(0, SIDES - 1)], ring_sem.at[0])
        for kz in FAR_Z:
            for core in (1, 0):
                push(ring, bundle, 0, ids_sem.at[z], z_peer(kz, core))
        push(ring, bundle, 0, ids_sem.at[z], other)
        pl.semaphore_signal(ready, inc=1, device_id=other, device_id_type=MESH)
        pltpu.make_async_copy(ring, bundle, ids_sem.at[z]).start()

    @pl.when(w == 0)
    def _():
        pl.semaphore_wait(ready, 1)

    wait(small.at[pl.ds(0, OWNERS - 1)], small_sem.at[0])
    my_block = small.at[pl.ds((far * NZ + z) * SIDES, SIDES)]
    my_column = small.at[pl.ds(far * NZ * SIDES, NZ * SIDES)]
    for kz in FAR_Z:
        push(my_block, my_block, 3, small_sem.at[1], z_peer(kz, w))

    lane = lax.broadcasted_iota(jnp.int32, (1, 128), 1)
    low_half = lane < 64
    low_half16 = lax.broadcasted_iota(jnp.int32, (16, 128), 1) < 64
    low_rows = lax.broadcasted_iota(jnp.int32, (LOW, WIDE), 0)

    for plane in range(NZ):
        wait(ids.at[pl.ds(plane * SIDES, SIDES)], ids_sem.at[plane])
        lines = [ids[pl.ds(plane * SIDES + near_line(side), 1), :] for side in range(SIDES)]
        wanted = jnp.concatenate(
            [jnp.where(low_half, a, b) for a, b in zip(lines[::2], lines[1::2])], axis=1
        )
        high = wanted >> 8
        hot = jnp.where(low_rows == (wanted & (LOW - 1)), 1.0, 0.0).astype(jnp.bfloat16)
        rows = jnp.zeros((F, WIDE), jnp.float32)
        for slots in ((0, 1, 2), (3,)) if plane == 0 else ((0, 1), (2, 3)):
            if plane == 0:
                first = max(slots[0], 1)
                wait(tab.at[pl.ds(first, slots[-1] - first + 1)], tab_sem.at[first // 3])
            lhs = jnp.concatenate(
                [tab[j, :, b * LOW : (b + 1) * LOW] for j in slots for b in range(HIGH)], axis=0
            )
            found = jnp.dot(lhs, hot, preferred_element_type=jnp.float32)
            at = 0
            for j in slots:
                yo, xo = owner(j)
                for b in range(HIGH):
                    here = ((z * NY + yo) * NX + xo) * HIGH + b
                    rows = jnp.where(high == here, found[at : at + F], rows)
                    at += F
        for half in range(SIDES // 2):
            part = rows[:, half * 128 : (half + 1) * 128]
            upper, lower = part[:16], part[16:]
            turned_upper = pltpu.roll(upper, 64, 1)
            turned_lower = pltpu.roll(lower, 64, 1)
            slot = plane * SIDES + 2 * half
            send[slot] = jnp.where(low_half16, upper, turned_lower).astype(jnp.bfloat16)
            send[slot + 1] = jnp.where(low_half16, turned_upper, lower).astype(jnp.bfloat16)
        for side in FAR_SIDE:
            source, target = send.at[plane * SIDES + side], recv.at[block]
            if side:
                push(source, target, 2, row_sem.at[0], near_peer(plane, side, w))
                continue

            @pl.when(plane != z)
            def _():
                push(source, target, 2, row_sem.at[0], near_peer(plane, side, w))

            @pl.when(plane == z)
            def _():
                pltpu.make_async_copy(source, target, row_sem.at[0]).start()

        if plane == 3:
            wait(small.at[pl.ds(0, OWNERS * (NZ - 1))], small_sem.at[1])
            for slot in range(1, OWNERS):
                push(my_column, my_column, 3, small_sem.at[2], gather_peer(slot, w))

    @pl.when(w == 1)
    def _():
        wait(ids.at[pl.ds(0, PEERS)], send_sem.at[0])
        wait(ids.at[pl.ds(0, PEERS - 1)], send_sem.at[0])

    wait(tab.at[pl.ds(1, OWNERS - 1)], send_sem.at[1])
    wait(small.at[pl.ds(0, OWNERS * PEERS - 1)], send_sem.at[3])
    wait(send.at[pl.ds(1, PEERS - 1)], send_sem.at[2])
    wait(recv.at[pl.ds(0, PEERS)], row_sem.at[0])
    wait(small.at[pl.ds(0, OWNERS * NZ * (SIDES - 1))], small_sem.at[2])
    wanted = sid[...]
    device = wanted >> 1
    high_bits = device >> 1
    folded = device ^ high_bits
    column = ((folded >> 1) & 2) | (folded & 1)
    line = ((((high_bits >> 1) & 2) | (high_bits & 1)) * NZ + (device >> 4)) * SIDES + column
    lines = small[...].astype(jnp.bfloat16)
    small_rows = jnp.zeros((EX, F), jnp.float32)
    for row in range(2):
        spot = jnp.where((wanted & 1) == row, line, -1)
        small_hot = jnp.where(
            lax.broadcasted_iota(jnp.int32, (OWNERS * PEERS, EX), 0) == spot, 1.0, 0.0
        ).astype(jnp.bfloat16)
        small_rows = small_rows + lax.dot_general(
            small_hot, lines[:, row * F : (row + 1) * F], (((0,), (0,)), ((), ())),
            preferred_element_type=jnp.float32,
        )
    out_ref[2] = small_rows.astype(jnp.bfloat16)

    blocks = [recv[slot] for slot in range(PEERS)]
    while len(blocks) > 1:
        blocks = [a + b for a, b in zip(blocks[::2], blocks[1::2])]
    total = blocks[0].astype(jnp.float32)
    both = jnp.concatenate(
        [jnp.where(low_half16, total, 0.0), jnp.where(low_half16, 0.0, total)], axis=0
    ).astype(jnp.bfloat16)
    example = lax.broadcasted_iota(jnp.int32, (EX, 128), 0)
    spot = lax.broadcasted_iota(jnp.int32, (EX, 128), 1)
    picks = jnp.where((spot & (EX - 1)) == example, 1.0, 0.0).astype(jnp.bfloat16)
    pooled = lax.dot_general(
        picks, both, (((1,), (1,)), ((), ())), preferred_element_type=jnp.float32
    )
    out_ref[1] = (pooled * 2 ** (-0.5)).astype(jnp.bfloat16)


def shards(row_numbers, item_table, dense_part, small_ids, small_table):
    dma = pltpu.SemaphoreType.DMA
    arrays = row_numbers.T, item_table.T, dense_part, small_ids.reshape(1, EX), small_table
    parts = pl.pallas_call(
        kernel,
        out_shape=jax.ShapeDtypeStruct((3, EX, F), jnp.bfloat16),
        in_specs=[pl.BlockSpec(memory_space=pltpu.HBM)] * 5,
        out_specs=pl.BlockSpec(memory_space=pltpu.VMEM),
        scratch_shapes=[
            pltpu.VMEM((2, EX), jnp.int32),
            pltpu.VMEM((EX, F), jnp.float32),
            pltpu.VMEM((1, EX), jnp.int32),
            pltpu.VMEM((2, F), jnp.bfloat16),
            pltpu.VMEM((SIDES, 128), jnp.int32),
            pltpu.VMEM((PEERS, 128), jnp.int32),
            pltpu.VMEM((OWNERS, F, ROWS), jnp.bfloat16),
            pltpu.VMEM((PEERS, 16, 128), jnp.bfloat16),
            pltpu.VMEM((PEERS, 16, 128), jnp.bfloat16),
            pltpu.VMEM((OWNERS * PEERS, 128), jnp.float32),
            dma((5,)), dma((4,)), dma((2,)), dma((1,)), dma((NZ,)), dma((1,)), dma((3,)),
            pltpu.SemaphoreType.REGULAR,
        ],
        compiler_params=pltpu.CompilerParams(
            collective_id=0, has_side_effects=True, vmem_limit_bytes=16 * 2**20
        ),
    )(*(pltpu.with_memory_space_constraint(array, pltpu.HBM) for array in arrays))
    return parts.transpose(1, 0, 2)


def solution(mesh):
    torus = Mesh(mesh.devices.reshape(NZ, NY, NX, 2), (*ROW, "width"))
    return jax.shard_map(
        shards,
        mesh=torus,
        in_specs=(P(ROW, None), P(ROW, "width"), P(ROW, "width"), P(ROW), P(ROW, "width")),
        out_specs=P(ROW, None, "width"),
        check_vma=False,
    )
```

```python
import jax
import jax.numpy as jnp
from jax import lax
from jax.experimental import pallas as pl
from jax.experimental.pallas import tpu as pltpu
from jax.sharding import Mesh
from jax.sharding import PartitionSpec as P

ROW = ("row_0", "row_1", "row_2")
NZ, NY, NX = 8, 4, 4
MESH = pl.DeviceIdType.MESH
BLOCKS = ((0, 0), (0, 1), (1, 0), (1, 1))
OWNERS = len(BLOCKS)
SIDES = len(BLOCKS)
PEERS = NZ * SIDES
FAR_Z = (4, 3, 5, 2, 6, 1, 7)
FAR_SIDE = (3, 1, 2, 0)
ROWS = 1024
LOW = 256
HIGH = ROWS // LOW
EX = 32
F = 32
WIDE = SIDES * 64


def kernel(
    ids_hbm, table_hbm, dense_hbm, sid_hbm, small_hbm, out_ref,
    ids_in, dense, sid, small_in, ring, ids, tab, send, recv, small,
    local_sem, send_sem, tab_sem, ring_sem, ids_sem, row_sem, small_sem, ready,
):
    z, y, x, w = (lax.axis_index(name) for name in (*ROW, "width"))
    far_y, far_x = y // 2, x // 2
    half_y, half_x = y + far_y * (3 - 2 * y), x + far_x * (3 - 2 * x)
    quarter = half_y * 2 + half_x
    block = z * SIDES + quarter

    def owner(slot):
        fy, fx = BLOCKS[slot]
        return NY - 1 - y if fy else y, NX - 1 - x if fx else x

    part = z - z // 4 * (z - 4)

    def gather_peer(slot, core):
        return (z, *owner(slot), core)

    def near_peer(plane, side, core):
        my, mx = BLOCKS[side]
        return (
            plane,
            y + 1 - 2 * lax.rem(y, 2) if my else y,
            x + 1 - 2 * lax.rem(x, 2) if mx else x,
            core,
        )

    def near_line(side):
        my, mx = BLOCKS[side]
        return (1 - half_y if my else half_y) * 2 + (1 - half_x if mx else half_x)

    def z_peer(kz, core):
        return (lax.rem(z + kz, NZ), y, x, core)

    barrier = pltpu.get_barrier_semaphore()
    other = (z, y, x, 1 - w)
    for slot in range(1, OWNERS):
        pl.semaphore_signal(barrier, inc=1, device_id=gather_peer(slot, 0), device_id_type=MESH)
    pl.semaphore_signal(barrier, inc=1, device_id=other, device_id_type=MESH)

    for side in range(1, SIDES):
        pl.semaphore_signal(barrier, inc=1, device_id=near_peer(z, side, 0), device_id_type=MESH)
    for kz in FAR_Z:
        pl.semaphore_signal(barrier, inc=1, device_id=z_peer(kz, 1), device_id_type=MESH)

    fetches = [
        pltpu.make_async_copy(src, dst, local_sem.at[i])
        for i, (src, dst) in enumerate(
            (
                (table_hbm, tab.at[0]), (small_hbm, small_in), (ids_hbm, ids_in),
                (sid_hbm, sid), (dense_hbm, dense),
            )
        )
    ]
    for fetch in fetches:
        fetch.start()

    def push(src, dst, kind, sem, peer):
        pltpu.make_async_remote_copy(
            src_ref=src, dst_ref=dst, send_sem=send_sem.at[kind], recv_sem=sem,
            device_id=peer, device_id_type=MESH,
        ).start()

    def wait(ref, sem):
        pltpu.make_async_copy(ref, ref, sem).wait()

    fetches[1].wait()
    two = small_in[...].astype(jnp.float32)
    far = far_y * 2 + far_x
    my_line = small.at[pl.ds((far * NZ + z) * SIDES + quarter, 1)]
    my_line[...] = jnp.concatenate([two[0:1], two[1:2], two[0:1], two[1:2]], axis=1)
    fetches[2].wait()
    pair = ids_in[...]
    line = jnp.concatenate([pair[0:1], pair[1:2], pair[0:1], pair[1:2]], axis=1)
    my_ring = ring.at[pl.ds(quarter, 1)]
    my_ring[...] = line
    fetches[0].wait()
    fetches[3].wait()
    fetches[4].wait()
    out_ref[0] = dense[...].astype(jnp.bfloat16)

    @pl.when(w == 0)
    def _():
        pl.semaphore_wait(barrier, 2 * (OWNERS + SIDES - 2) + 1)
        pl.semaphore_signal(ready, inc=1, device_id=other, device_id_type=MESH)

    @pl.when(w == 1)
    def _():
        pl.semaphore_wait(ready, 1)
        for side in FAR_SIDE[:-1]:
            push(my_ring, my_ring, 0, ring_sem.at[0], near_peer(z, side, 1))

    for side in range(1, SIDES):
        push(my_line, my_line, 3, small_sem.at[0], near_peer(z, side, w))
    for slot in range(OWNERS - 1, 0, -1):
        push(tab.at[0], tab.at[slot], 1, tab_sem.at[slot // 3], gather_peer(slot, w))

    @pl.when(w == 1)
    def _():
        bundle = ids.at[pl.ds(z * SIDES, SIDES)]
        pl.semaphore_wait(barrier, 2 * (NZ - 1) + 1)
        wait(ring.at[pl.ds(0, SIDES - 1)], ring_sem.at[0])
        for kz in FAR_Z:
            for core in (1, 0):
                push(ring, bundle, 0, ids_sem.at[part], z_peer(kz, core))
        push(ring, bundle, 0, ids_sem.at[part], other)
        pl.semaphore_signal(ready, inc=1, device_id=other, device_id_type=MESH)
        pltpu.make_async_copy(ring, bundle, ids_sem.at[part]).start()

    @pl.when(w == 0)
    def _():
        pl.semaphore_wait(ready, 1)

    wait(small.at[pl.ds(0, OWNERS - 1)], small_sem.at[0])
    my_block = small.at[pl.ds((far * NZ + z) * SIDES, SIDES)]
    my_column = small.at[pl.ds(far * NZ * SIDES, NZ * SIDES)]
    for kz in FAR_Z:
        push(my_block, my_block, 3, small_sem.at[1], z_peer(kz, w))

    lane = lax.broadcasted_iota(jnp.int32, (1, 128), 1)
    low_half = lane < 64
    low_half16 = lax.broadcasted_iota(jnp.int32, (16, 128), 1) < 64
    low_rows = lax.broadcasted_iota(jnp.int32, (LOW, WIDE), 0)

    for plane in range(NZ):
        if plane <= 4:
            planes = 1 if plane < 4 else NZ - 4
            wait(ids.at[pl.ds(plane * SIDES, planes * SIDES)], ids_sem.at[plane])
        lines = [ids[pl.ds(plane * SIDES + near_line(side), 1), :] for side in range(SIDES)]
        wanted = jnp.concatenate(
            [jnp.where(low_half, a, b) for a, b in zip(lines[::2], lines[1::2])], axis=1
        )
        high = wanted >> 8
        hot = jnp.where(low_rows == (wanted & (LOW - 1)), 1.0, 0.0).astype(jnp.bfloat16)
        rows = jnp.zeros((F, WIDE), jnp.float32)
        for slots in ((0, 1, 2), (3,)) if plane == 0 else ((0, 1), (2, 3)):
            if plane == 0:
                first = max(slots[0], 1)
                wait(tab.at[pl.ds(first, slots[-1] - first + 1)], tab_sem.at[first // 3])
            lhs = jnp.concatenate(
                [tab[j, :, b * LOW : (b + 1) * LOW] for j in slots for b in range(HIGH)], axis=0
            )
            found = jnp.dot(lhs, hot, preferred_element_type=jnp.float32)
            at = 0
            for j in slots:
                yo, xo = owner(j)
                for b in range(HIGH):
                    here = ((z * NY + yo) * NX + xo) * HIGH + b
                    rows = jnp.where(high == here, found[at : at + F], rows)
                    at += F
        for half in range(SIDES // 2):
            part = rows[:, half * 128 : (half + 1) * 128]
            upper, lower = part[:16], part[16:]
            turned_upper = pltpu.roll(upper, 64, 1)
            turned_lower = pltpu.roll(lower, 64, 1)
            slot = plane * SIDES + 2 * half
            send[slot] = jnp.where(low_half16, upper, turned_lower).astype(jnp.bfloat16)
            send[slot + 1] = jnp.where(low_half16, turned_upper, lower).astype(jnp.bfloat16)
        for side in FAR_SIDE:
            source, target = send.at[plane * SIDES + side], recv.at[block]
            if side:
                push(source, target, 2, row_sem.at[0], near_peer(plane, side, w))
                continue

            @pl.when(plane != z)
            def _():
                push(source, target, 2, row_sem.at[0], near_peer(plane, side, w))

            @pl.when(plane == z)
            def _():
                pltpu.make_async_copy(source, target, row_sem.at[0]).start()

        if plane == 3:
            wait(small.at[pl.ds(0, OWNERS * (NZ - 1))], small_sem.at[1])
            for slot in range(1, OWNERS):
                push(my_column, my_column, 3, small_sem.at[2], gather_peer(slot, w))

    @pl.when(w == 1)
    def _():
        wait(ids.at[pl.ds(0, PEERS)], send_sem.at[0])
        wait(ids.at[pl.ds(0, PEERS - 1)], send_sem.at[0])

    wait(tab.at[pl.ds(1, OWNERS - 1)], send_sem.at[1])
    wait(small.at[pl.ds(0, OWNERS * PEERS - 1)], send_sem.at[3])
    wait(send.at[pl.ds(1, PEERS - 1)], send_sem.at[2])
    wait(recv.at[pl.ds(0, PEERS)], row_sem.at[0])
    wait(small.at[pl.ds(0, OWNERS * NZ * (SIDES - 1))], small_sem.at[2])
    wanted = sid[...]
    device = wanted >> 1
    high_bits = device >> 1
    folded = device ^ high_bits
    column = ((folded >> 1) & 2) | (folded & 1)
    line = ((((high_bits >> 1) & 2) | (high_bits & 1)) * NZ + (device >> 4)) * SIDES + column
    lines = small[...].astype(jnp.bfloat16)
    small_rows = jnp.zeros((EX, F), jnp.float32)
    for row in range(2):
        spot = jnp.where((wanted & 1) == row, line, -1)
        small_hot = jnp.where(
            lax.broadcasted_iota(jnp.int32, (OWNERS * PEERS, EX), 0) == spot, 1.0, 0.0
        ).astype(jnp.bfloat16)
        small_rows = small_rows + lax.dot_general(
            small_hot, lines[:, row * F : (row + 1) * F], (((0,), (0,)), ((), ())),
            preferred_element_type=jnp.float32,
        )
    out_ref[2] = small_rows.astype(jnp.bfloat16)

    blocks = [recv[slot] for slot in range(PEERS)]
    while len(blocks) > 1:
        blocks = [a + b for a, b in zip(blocks[::2], blocks[1::2])]
    total = blocks[0].astype(jnp.float32)
    both = jnp.concatenate(
        [jnp.where(low_half16, total, 0.0), jnp.where(low_half16, 0.0, total)], axis=0
    ).astype(jnp.bfloat16)
    example = lax.broadcasted_iota(jnp.int32, (EX, 128), 0)
    spot = lax.broadcasted_iota(jnp.int32, (EX, 128), 1)
    picks = jnp.where((spot & (EX - 1)) == example, 1.0, 0.0).astype(jnp.bfloat16)
    pooled = lax.dot_general(
        picks, both, (((1,), (1,)), ((), ())), preferred_element_type=jnp.float32
    )
    out_ref[1] = (pooled * 2 ** (-0.5)).astype(jnp.bfloat16)


def shards(row_numbers, item_table, dense_part, small_ids, small_table):
    dma = pltpu.SemaphoreType.DMA
    arrays = row_numbers.T, item_table.T, dense_part, small_ids.reshape(1, EX), small_table
    parts = pl.pallas_call(
        kernel,
        out_shape=jax.ShapeDtypeStruct((3, EX, F), jnp.bfloat16),
        in_specs=[pl.BlockSpec(memory_space=pltpu.HBM)] * 5,
        out_specs=pl.BlockSpec(memory_space=pltpu.VMEM),
        scratch_shapes=[
            pltpu.VMEM((2, EX), jnp.int32),
            pltpu.VMEM((EX, F), jnp.float32),
            pltpu.VMEM((1, EX), jnp.int32),
            pltpu.VMEM((2, F), jnp.bfloat16),
            pltpu.VMEM((SIDES, 128), jnp.int32),
            pltpu.VMEM((PEERS, 128), jnp.int32),
            pltpu.VMEM((OWNERS, F, ROWS), jnp.bfloat16),
            pltpu.VMEM((PEERS, 16, 128), jnp.bfloat16),
            pltpu.VMEM((PEERS, 16, 128), jnp.bfloat16),
            pltpu.VMEM((OWNERS * PEERS, 128), jnp.float32),
            dma((5,)), dma((4,)), dma((2,)), dma((1,)), dma((5,)), dma((1,)), dma((3,)),
            pltpu.SemaphoreType.REGULAR,
        ],
        compiler_params=pltpu.CompilerParams(
            collective_id=0, has_side_effects=True, vmem_limit_bytes=16 * 2**20
        ),
    )(*(pltpu.with_memory_space_constraint(array, pltpu.HBM) for array in arrays))
    return parts.transpose(1, 0, 2)


def solution(mesh):
    torus = Mesh(mesh.devices.reshape(NZ, NY, NX, 2), (*ROW, "width"))
    return jax.shard_map(
        shards,
        mesh=torus,
        in_specs=(P(ROW, None), P(ROW, "width"), P(ROW, "width"), P(ROW), P(ROW, "width")),
        out_specs=P(ROW, None, "width"),
        check_vma=False,
    )
```

```python
import jax
import jax.numpy as jnp
from jax import lax
from jax.experimental import pallas as pl
from jax.experimental.pallas import tpu as pltpu
from jax.sharding import Mesh
from jax.sharding import PartitionSpec as P

ROW = ("row_0", "row_1", "row_2")
NZ, NY, NX = 8, 4, 4
MESH = pl.DeviceIdType.MESH
BLOCKS = ((0, 0), (0, 1), (1, 0), (1, 1))
OWNERS = len(BLOCKS)
SIDES = len(BLOCKS)
PEERS = NZ * SIDES
FAR_Z = (4, 3, 5, 2, 6, 1, 7)
FAR_SIDE = (3, 1, 2, 0)
ROWS = 1024
LOW = 256
HIGH = ROWS // LOW
EX = 32
F = 32
WIDE = SIDES * 64


def kernel(
    ids_hbm, table_hbm, dense_hbm, sid_hbm, small_hbm, out_ref,
    ids_in, dense, sid, small_in, ring, ids, tab, send, recv, small,
    local_sem, send_sem, tab_sem, ring_sem, ids_sem, row_sem, small_sem, ready,
):
    z, y, x, w = (lax.axis_index(name) for name in (*ROW, "width"))
    far_y, far_x = y // 2, x // 2
    half_y, half_x = y + far_y * (3 - 2 * y), x + far_x * (3 - 2 * x)
    quarter = half_y * 2 + half_x
    block = z * SIDES + quarter

    def owner(slot):
        fy, fx = BLOCKS[slot]
        return NY - 1 - y if fy else y, NX - 1 - x if fx else x

    def gather_peer(slot, core):
        return (z, *owner(slot), core)

    def near_peer(plane, side, core):
        my, mx = BLOCKS[side]
        return (
            plane,
            y + 1 - 2 * lax.rem(y, 2) if my else y,
            x + 1 - 2 * lax.rem(x, 2) if mx else x,
            core,
        )

    def near_line(side):
        my, mx = BLOCKS[side]
        return (1 - half_y if my else half_y) * 2 + (1 - half_x if mx else half_x)

    def z_peer(kz, core):
        return (lax.rem(z + kz, NZ), y, x, core)

    barrier = pltpu.get_barrier_semaphore()
    other = (z, y, x, 1 - w)
    for kz in FAR_Z:
        pl.semaphore_signal(barrier, inc=1, device_id=z_peer(kz, 1), device_id_type=MESH)
    for slot in range(1, OWNERS):
        pl.semaphore_signal(barrier, inc=1, device_id=gather_peer(slot, 0), device_id_type=MESH)
    pl.semaphore_signal(barrier, inc=1, device_id=other, device_id_type=MESH)

    for side in range(1, SIDES):
        pl.semaphore_signal(barrier, inc=1, device_id=near_peer(z, side, 0), device_id_type=MESH)


    fetches = [
        pltpu.make_async_copy(src, dst, local_sem.at[i])
        for i, (src, dst) in enumerate(
            (
                (table_hbm, tab.at[0]), (small_hbm, small_in), (ids_hbm, ids_in),
                (sid_hbm, sid), (dense_hbm, dense),
            )
        )
    ]
    for fetch in fetches:
        fetch.start()

    def push(src, dst, kind, sem, peer):
        pltpu.make_async_remote_copy(
            src_ref=src, dst_ref=dst, send_sem=send_sem.at[kind], recv_sem=sem,
            device_id=peer, device_id_type=MESH,
        ).start()

    def wait(ref, sem):
        pltpu.make_async_copy(ref, ref, sem).wait()

    fetches[1].wait()
    two = small_in[...].astype(jnp.float32)
    far = far_y * 2 + far_x
    my_line = small.at[pl.ds((far * NZ + z) * SIDES + quarter, 1)]
    my_line[...] = jnp.concatenate([two[0:1], two[1:2], two[0:1], two[1:2]], axis=1)
    fetches[2].wait()
    pair = ids_in[...]
    line = jnp.concatenate([pair[0:1], pair[1:2], pair[0:1], pair[1:2]], axis=1)
    my_ring = ring.at[pl.ds(quarter, 1)]
    my_ring[...] = line
    fetches[0].wait()
    fetches[3].wait()
    fetches[4].wait()
    out_ref[0] = dense[...].astype(jnp.bfloat16)

    @pl.when(w == 0)
    def _():
        pl.semaphore_wait(barrier, 2 * (OWNERS + SIDES - 2) + 1)
        pl.semaphore_signal(ready, inc=1, device_id=other, device_id_type=MESH)

    @pl.when(w == 1)
    def _():
        pl.semaphore_wait(ready, 1)
        for side in FAR_SIDE[:-1]:
            push(my_ring, my_ring, 0, ring_sem.at[0], near_peer(z, side, 1))

    for slot in range(OWNERS - 1, 0, -1):
        push(tab.at[0], tab.at[slot], 1, tab_sem.at[slot // 3], gather_peer(slot, w))
    for side in range(1, SIDES):
        push(my_line, my_line, 3, small_sem.at[0], near_peer(z, side, w))

    @pl.when(w == 1)
    def _():
        bundle = ids.at[pl.ds(z * SIDES, SIDES)]
        pl.semaphore_wait(barrier, 2 * (NZ - 1) + 1)
        wait(ring.at[pl.ds(0, SIDES - 1)], ring_sem.at[0])
        for kz in FAR_Z:
            for core in (1, 0):
                push(ring, bundle, 0, ids_sem.at[z], z_peer(kz, core))
        push(ring, bundle, 0, ids_sem.at[z], other)
        pl.semaphore_signal(ready, inc=1, device_id=other, device_id_type=MESH)
        pltpu.make_async_copy(ring, bundle, ids_sem.at[z]).start()

    @pl.when(w == 0)
    def _():
        pl.semaphore_wait(ready, 1)

    wait(small.at[pl.ds(0, OWNERS - 1)], small_sem.at[0])
    my_block = small.at[pl.ds((far * NZ + z) * SIDES, SIDES)]
    my_column = small.at[pl.ds(far * NZ * SIDES, NZ * SIDES)]
    for kz in FAR_Z:
        push(my_block, my_block, 3, small_sem.at[1], z_peer(kz, w))

    lane = lax.broadcasted_iota(jnp.int32, (1, 128), 1)
    low_half = lane < 64
    low_half16 = lax.broadcasted_iota(jnp.int32, (16, 128), 1) < 64
    low_rows = lax.broadcasted_iota(jnp.int32, (LOW, WIDE), 0)

    for plane in range(NZ):
        wait(ids.at[pl.ds(plane * SIDES, SIDES)], ids_sem.at[plane])
        lines = [ids[pl.ds(plane * SIDES + near_line(side), 1), :] for side in range(SIDES)]
        wanted = jnp.concatenate(
            [jnp.where(low_half, a, b) for a, b in zip(lines[::2], lines[1::2])], axis=1
        )
        high = wanted >> 8
        hot = jnp.where(low_rows == (wanted & (LOW - 1)), 1.0, 0.0).astype(jnp.bfloat16)
        rows = jnp.zeros((F, WIDE), jnp.float32)
        for slots in ((0, 1, 2), (3,)) if plane == 0 else ((0, 1), (2, 3)):
            if plane == 0:
                first = max(slots[0], 1)
                wait(tab.at[pl.ds(first, slots[-1] - first + 1)], tab_sem.at[first // 3])
            lhs = jnp.concatenate(
                [tab[j, :, b * LOW : (b + 1) * LOW] for j in slots for b in range(HIGH)], axis=0
            )
            found = jnp.dot(lhs, hot, preferred_element_type=jnp.float32)
            at = 0
            for j in slots:
                yo, xo = owner(j)
                for b in range(HIGH):
                    here = ((z * NY + yo) * NX + xo) * HIGH + b
                    rows = jnp.where(high == here, found[at : at + F], rows)
                    at += F
        for half in range(SIDES // 2):
            part = rows[:, half * 128 : (half + 1) * 128]
            upper, lower = part[:16], part[16:]
            turned_upper = pltpu.roll(upper, 64, 1)
            turned_lower = pltpu.roll(lower, 64, 1)
            slot = plane * SIDES + 2 * half
            send[slot] = jnp.where(low_half16, upper, turned_lower).astype(jnp.bfloat16)
            send[slot + 1] = jnp.where(low_half16, turned_upper, lower).astype(jnp.bfloat16)
        for side in FAR_SIDE:
            source, target = send.at[plane * SIDES + side], recv.at[block]
            if side:
                push(source, target, 2, row_sem.at[0], near_peer(plane, side, w))
                continue

            @pl.when(plane != z)
            def _():
                push(source, target, 2, row_sem.at[0], near_peer(plane, side, w))

            @pl.when(plane == z)
            def _():
                pltpu.make_async_copy(source, target, row_sem.at[0]).start()

        if plane == 3:
            wait(small.at[pl.ds(0, OWNERS * (NZ - 1))], small_sem.at[1])
            for slot in range(1, OWNERS):
                push(my_column, my_column, 3, small_sem.at[2], gather_peer(slot, w))

    @pl.when(w == 1)
    def _():
        wait(ids.at[pl.ds(0, PEERS)], send_sem.at[0])
        wait(ids.at[pl.ds(0, PEERS - 1)], send_sem.at[0])

    wait(tab.at[pl.ds(1, OWNERS - 1)], send_sem.at[1])
    wait(small.at[pl.ds(0, OWNERS * PEERS - 1)], send_sem.at[3])
    wait(send.at[pl.ds(1, PEERS - 1)], send_sem.at[2])
    wait(recv.at[pl.ds(0, PEERS)], row_sem.at[0])
    wait(small.at[pl.ds(0, OWNERS * NZ * (SIDES - 1))], small_sem.at[2])
    wanted = sid[...]
    device = wanted >> 1
    high_bits = device >> 1
    folded = device ^ high_bits
    column = ((folded >> 1) & 2) | (folded & 1)
    line = ((((high_bits >> 1) & 2) | (high_bits & 1)) * NZ + (device >> 4)) * SIDES + column
    lines = small[...].astype(jnp.bfloat16)
    small_rows = jnp.zeros((EX, F), jnp.float32)
    for row in range(2):
        spot = jnp.where((wanted & 1) == row, line, -1)
        small_hot = jnp.where(
            lax.broadcasted_iota(jnp.int32, (OWNERS * PEERS, EX), 0) == spot, 1.0, 0.0
        ).astype(jnp.bfloat16)
        small_rows = small_rows + lax.dot_general(
            small_hot, lines[:, row * F : (row + 1) * F], (((0,), (0,)), ((), ())),
            preferred_element_type=jnp.float32,
        )
    out_ref[2] = small_rows.astype(jnp.bfloat16)

    total = recv[0].astype(jnp.float32)
    for slot in range(1, PEERS):
        total = total + recv[slot].astype(jnp.float32)
    both = jnp.concatenate(
        [jnp.where(low_half16, total, 0.0), jnp.where(low_half16, 0.0, total)], axis=0
    ).astype(jnp.bfloat16)
    example = lax.broadcasted_iota(jnp.int32, (EX, 128), 0)
    spot = lax.broadcasted_iota(jnp.int32, (EX, 128), 1)
    picks = jnp.where((spot & (EX - 1)) == example, 1.0, 0.0).astype(jnp.bfloat16)
    pooled = lax.dot_general(
        picks, both, (((1,), (1,)), ((), ())), preferred_element_type=jnp.float32
    )
    out_ref[1] = (pooled * 2 ** (-0.5)).astype(jnp.bfloat16)


def shards(row_numbers, item_table, dense_part, small_ids, small_table):
    dma = pltpu.SemaphoreType.DMA
    arrays = row_numbers.T, item_table.T, dense_part, small_ids.reshape(1, EX), small_table
    parts = pl.pallas_call(
        kernel,
        out_shape=jax.ShapeDtypeStruct((3, EX, F), jnp.bfloat16),
        in_specs=[pl.BlockSpec(memory_space=pltpu.HBM)] * 5,
        out_specs=pl.BlockSpec(memory_space=pltpu.VMEM),
        scratch_shapes=[
            pltpu.VMEM((2, EX), jnp.int32),
            pltpu.VMEM((EX, F), jnp.float32),
            pltpu.VMEM((1, EX), jnp.int32),
            pltpu.VMEM((2, F), jnp.bfloat16),
            pltpu.VMEM((SIDES, 128), jnp.int32),
            pltpu.VMEM((PEERS, 128), jnp.int32),
            pltpu.VMEM((OWNERS, F, ROWS), jnp.bfloat16),
            pltpu.VMEM((PEERS, 16, 128), jnp.bfloat16),
            pltpu.VMEM((PEERS, 16, 128), jnp.bfloat16),
            pltpu.VMEM((OWNERS * PEERS, 128), jnp.float32),
            dma((5,)), dma((4,)), dma((2,)), dma((1,)), dma((NZ,)), dma((1,)), dma((3,)),
            pltpu.SemaphoreType.REGULAR,
        ],
        compiler_params=pltpu.CompilerParams(
            collective_id=0, has_side_effects=True, vmem_limit_bytes=16 * 2**20
        ),
    )(*(pltpu.with_memory_space_constraint(array, pltpu.HBM) for array in arrays))
    return parts.transpose(1, 0, 2)


def solution(mesh):
    torus = Mesh(mesh.devices.reshape(NZ, NY, NX, 2), (*ROW, "width"))
    return jax.shard_map(
        shards,
        mesh=torus,
        in_specs=(P(ROW, None), P(ROW, "width"), P(ROW, "width"), P(ROW), P(ROW, "width")),
        out_specs=P(ROW, None, "width"),
        check_vma=False,
    )
```
